256 devices in a mesh: gx: 8 (over z), gy: 32 (over x, y, core).
Axes of the slice: x: 4, y: 4, z: 8, core: 2. Of those that a mesh axis runs over, the one named last changes fastest.
Arguments:
- features: bfloat16 [65536, 512], P(('gx', 'gy')), may hold values from -24 to 24
- cotangent: bfloat16 [65536, 512], P(('gx', 'gy')), may hold values from -24 to 24
- self_weight: bfloat16 [3, 512, 512], replicated, may hold values from -0.25 to 0.25
- neigh_weight: bfloat16 [3, 512, 512], replicated, may hold values from -0.25 to 0.25
- block_val: bfloat16 [512, 4, 128, 128], P(('gx', 'gy')), may hold values from -0.25 to 0.25
- block_col: int32 [512, 4], P(('gx', 'gy')), may hold values from 0 to 5
- send_idx: int32 [256, 256, 2], P(('gx', 'gy')), may hold values from 0 to 255
- send_count: int32 [256, 256], P(('gx', 'gy')), may hold values from 0 to 2, as said below
Outputs:
- self_grad: bfloat16 [3, 512, 512], replicated
- neigh_grad: bfloat16 [3, 512, 512], replicated
- input_grad: bfloat16 [65536, 512], P(('gx', 'gy'))
The draws below stay inside these ranges and needn't reach their ends.
Inputs may be any that keep to these rules, and one draw needn't show every extreme that they name: `send_count`: at most 2 rows from one device to one peer; in every draw some receivers get exactly 2 from every device.
All inputs are finite; a program needn't handle non-finite values.
Results may differ from the reference program's by a relative error of at most 0.02.
Values may be sent and summed in bfloat16 or wider, within the bound.
A program may use at most 128 MiB of HBM per device.

```python
import math
import jax
import jax.numpy as jnp
from jax import lax

D = 512
TILE = 128
BPT = 4
LAYERS = 3
NODE_DEV = 256
HALO_DEV = 512
SLOT = 2
NODES = 65536
TILES_DEV = 2
EXT_TILES = 6
DEVICES = 256


def draw_send_count(key, part):
    base_key, hot_key = jax.random.split(jax.random.fold_in(key, 11))
    counts = jax.random.randint(base_key, (DEVICES, DEVICES), 0, SLOT + 1)
    ranks = jax.random.permutation(hot_key, DEVICES)
    hotset = ranks < max(DEVICES // 8, 1)
    return jnp.where(hotset[None, :], SLOT, counts).astype(jnp.int32)


def place_ends(result, rng, low, top_value):
    shape = result.shape
    place = [jax.random.randint(jax.random.fold_in(rng, axis), (), 0, shape[axis]) for axis in range(len(shape))]
    result = result.at[tuple(place)].set(low)
    longest = shape.index(max(shape))
    place[longest] = (place[longest] + 1) % shape[longest]
    return result.at[tuple(place)].set(top_value)


def spiked(drawn, key, source, target, parts, factor):
    def block_of(dim):
        return (jnp.arange(drawn.shape[dim]) // (drawn.shape[dim] // parts)).reshape((-1,) + (1,) * (drawn.ndim - 1 - dim))

    near = jax.random.permutation(key, parts)[block_of(target)]
    second = (block_of(target) + parts // 2) % parts
    return jnp.where((block_of(source) == near) | (block_of(source) == second), factor * drawn, drawn)


def shard_levels(stream_key, dims, cuts, least, largest):
    level, own = 1.0, jax.random.fold_in(stream_key, 6)
    for position, shards_of in cuts:
        draws = jnp.exp(jax.random.uniform(jax.random.fold_in(own, position), (shards_of,), jnp.float32, least / len(cuts), largest / len(cuts)))
        level = level * jnp.repeat(draws, dims[position] // shards_of).reshape([-1 if axis == position else 1 for axis in range(len(dims))])
    return level


def scatter_about(own_key, dims, scale, most, pieces=(), held_as=jnp.bfloat16):
    loudness = shard_levels(own_key, dims, pieces, -0.22, 0.18) if pieces else 1.0
    result = jax.random.normal(own_key, dims, jnp.float32) * scale * loudness
    return jnp.minimum(jnp.maximum(result, -most), most).astype(held_as)


def bell_draw_with(own_key, dims, deviation, most, cuts, heavy, kind=jnp.bfloat16):
    array = deviation * jax.random.normal(own_key, dims, jnp.float32)
    if cuts:
        array = array * shard_levels(own_key, dims, cuts, -0.22, 0.18)
    return jnp.clip(spiked(array, jax.random.fold_in(own_key, 3), *heavy), -most, most).astype(kind)


def setup_inputs(seed: int = 0) -> dict:
    arg_keys = jax.random.split(jax.random.key(seed), 9)
    return {
        "features": bell_draw_with(arg_keys[0], (NODES, D), 1.0, 24.0, ((0, 256),), (0, 1, 256, 6.0)),
        "cotangent": bell_draw_with(arg_keys[1], (NODES, D), 1.0, 24.0, ((0, 256),), (0, 1, 256, 6.0)),
        "self_weight": scatter_about(arg_keys[2], (LAYERS, D, D), D ** -0.5, 0.25),
        "neigh_weight": scatter_about(arg_keys[3], (LAYERS, D, D), D ** -0.5, 0.25),
        "block_val": scatter_about(arg_keys[4], (DEVICES * TILES_DEV, BPT, TILE, TILE), (BPT * TILE) ** -0.5, 0.25, ((0, 256),)),
        "block_col": place_ends(jax.random.randint(arg_keys[5], (DEVICES * TILES_DEV, BPT), 0, EXT_TILES), jax.random.fold_in(arg_keys[5], 1), 0, EXT_TILES - 1).astype(jnp.int32),
        "send_idx": place_ends(jax.random.randint(arg_keys[6], (DEVICES, DEVICES, SLOT), 0, NODE_DEV), jax.random.fold_in(arg_keys[6], 1), 0, NODE_DEV - 1).astype(jnp.int32),
        "send_count": draw_send_count(jax.random.fold_in(arg_keys[8], 71), 0),
    }


def reference(features, cotangent, self_weight, neigh_weight, block_val, block_col, send_idx, send_count):
    tiles_dev = NODE_DEV // TILE
    ext_tiles = (NODE_DEV + HALO_DEV) // TILE
    owners = (jnp.arange(DEVICES, dtype=jnp.int32)[:, None, None] * NODE_DEV + send_idx.astype(jnp.int32)).reshape(-1)
    live = (jnp.arange(SLOT, dtype=jnp.int32)[None, None, :] < send_count[:, :, None]).reshape(-1, 1)
    values = block_val.reshape(DEVICES, tiles_dev, BPT, TILE, TILE)
    columns = block_col.reshape(DEVICES, tiles_dev, BPT)
    scale = 1.0 / math.sqrt(NODES)

    def boundary(hidden):
        picked = jnp.where(live, hidden[owners], jnp.zeros((), hidden.dtype))
        picked = picked.reshape(DEVICES, DEVICES, SLOT, D).transpose(1, 0, 2, 3)
        return picked.reshape(DEVICES, HALO_DEV, D)

    def gather_sum(items):
        extended, vals, cols = items
        tiled = extended.reshape(ext_tiles, TILE, D)[cols]
        total = jnp.einsum('rbij,rbjd->rid', vals.astype(jnp.float32), tiled.astype(jnp.float32))
        return total.reshape(NODE_DEV, D)

    def spread(items):
        upstream, vals, cols = items
        contrib = jnp.einsum('rbij,rid->rbjd', vals.astype(jnp.float32), upstream.reshape(tiles_dev, TILE, D).astype(jnp.float32))
        total = jnp.zeros((ext_tiles, TILE, D), jnp.float32).at[cols.reshape(-1)].add(contrib.reshape(-1, TILE, D))
        return total.reshape(NODE_DEV + HALO_DEV, D)
    hiddens = [features]
    aggregates = []
    preacts = []
    hidden = features
    for layer_at in range(LAYERS):
        extended = jnp.concatenate([hidden.reshape(DEVICES, NODE_DEV, D), boundary(hidden)], axis=1)
        aggregate = lax.map(gather_sum, (extended, values, columns)).reshape(NODES, D).astype(jnp.bfloat16)
        preact = jnp.dot(hidden, self_weight[layer_at], preferred_element_type=jnp.float32) + jnp.dot(aggregate, neigh_weight[layer_at], preferred_element_type=jnp.float32)
        aggregates.append(aggregate)
        preacts.append(preact)
        if layer_at < LAYERS - 1:
            hidden = jax.nn.silu(preact).astype(jnp.bfloat16)
            hiddens.append(hidden)
    self_list = [None] * LAYERS
    neigh_list = [None] * LAYERS
    grad = cotangent
    for layer_at in reversed(range(LAYERS)):
        preact = preacts[layer_at]
        sigma = jax.nn.sigmoid(preact)
        delta = (grad.astype(jnp.float32) * sigma * (1.0 + preact * (1.0 - sigma))).astype(jnp.bfloat16)
        self_list[layer_at] = (jnp.dot(hiddens[layer_at].T, delta, preferred_element_type=jnp.float32) * scale).astype(jnp.bfloat16)
        neigh_list[layer_at] = (jnp.dot(aggregates[layer_at].T, delta, preferred_element_type=jnp.float32) * scale).astype(jnp.bfloat16)
        own_part = jnp.dot(delta, self_weight[layer_at].T, preferred_element_type=jnp.float32)
        upstream = jnp.dot(delta, neigh_weight[layer_at].T, preferred_element_type=jnp.float32).astype(jnp.bfloat16)
        ext_grad = lax.map(spread, (upstream.reshape(DEVICES, NODE_DEV, D), values, columns))
        halo_grad = ext_grad[:, NODE_DEV:].astype(jnp.bfloat16).reshape(DEVICES, DEVICES, SLOT, D)
        halo_grad = halo_grad.transpose(1, 0, 2, 3).reshape(-1, D)
        returned = jnp.zeros((NODES, D), jnp.float32).at[owners].add(jnp.where(live, halo_grad.astype(jnp.float32), jnp.zeros((), jnp.float32)))
        grad = (own_part + ext_grad[:, :NODE_DEV].reshape(NODES, D) + returned).astype(jnp.bfloat16)
    return (jnp.stack(self_list), jnp.stack(neigh_list), grad)
```

```python
import math

import jax
import jax.numpy as jnp
from jax import lax
from jax.experimental import pallas as pl
from jax.experimental.pallas import tpu as pltpu
from jax.sharding import PartitionSpec as P

MESH = pl.DeviceIdType.MESH
LANE = 128


def place():
    z, g = lax.axis_index("gx"), lax.axis_index("gy")
    x, y, c = g // 8, lax.rem(g // 2, 4), lax.rem(g, 2)
    return z, x, y, c


def flip(p, kind):
    return p + 1 - 2 * lax.rem(p, 2) if kind == 0 else 3 - p


def kept(p, kind):
    return lax.rem((p + 1) // 2, 2) if kind == 0 else p // 2


def rows(start, size):
    return pl.ds(pl.multiple_of(start, 16), size)


STEPS = (
    (("x", 0), ("x", 1), ("y", 0), ("y", 1)),
    (("x", 1), ("x", 0), ("y", 1), ("y", 0)),
    (("y", 0), ("y", 1), ("x", 0), ("x", 1)),
    (("y", 1), ("y", 0), ("x", 1), ("x", 0)),
)


def sum_kernel(
    scale, g_ref, out_ref, full, part, other, got, back, zin, zout, zgot, zall, ssem, rsem, zs, zr
):
    z, x, y, c = place()
    zn = 8
    n_mat, width = g_ref.shape[0], g_ref.shape[1]
    total = full.shape[0]
    half = total // 2
    colour = half // 4

    def at(x_, y_, c_):
        return (z, x_ * 8 + y_ * 2 + c_)

    def partner(axis, kind):
        return at(flip(x, kind), y, c) if axis == "x" else at(x, flip(y, kind), c)

    def keep(axis, kind):
        return kept(x if axis == "x" else y, kind)

    twin = at(x, y, 1 - c)
    bar = pltpu.get_barrier_semaphore()
    peers = [twin] + [partner(a, k) for a in "xy" for k in (0, 1)]
    peers += [(lax.rem(z + d, zn), x * 8 + y * 2 + c) for d in range(1, zn)]
    for peer in peers:
        pl.semaphore_signal(bar, inc=1, device_id=peer, device_id_type=MESH)

    blocks = width // LANE

    def load(i, carry):
        for k in range(blocks):
            full[rows((i * blocks + k) * width, width), :] = g_ref[
                i, :, k * LANE : (k + 1) * LANE
            ]
        return carry

    lax.fori_loop(0, n_mat, load, 0)
    pl.semaphore_wait(bar, len(peers))

    def copy(src, dst, s, r, peer):
        return pltpu.make_async_remote_copy(
            src_ref=src, dst_ref=dst, send_sem=s, recv_sem=r, device_id=peer, device_id_type=MESH
        )

    sends = []

    def go(*args):
        move = copy(*args)
        move.start()
        sends.append(move)

    for q in range(4):
        src = full.at[rows((1 - c) * half + q * colour, colour)]
        go(src, other.at[pl.ds(q * colour, colour)], ssem.at[q], rsem.at[q], twin)

    def add(dst, base, a, a_base, b, b_base, size):
        step = 96

        def body(i, carry):
            at_a = rows(a_base + i * step, step)
            at_b = rows(b_base + i * step, step)
            s = a[at_a, :].astype(jnp.float32) + b[at_b, :].astype(jnp.float32)
            dst[rows(base + i * step, step), :] = s.astype(jnp.bfloat16)
            return carry

        lax.fori_loop(0, size // step, body, 0)

    offset = [None] * 4
    got_at = [0, 4 * 768, 4 * 768 + 4 * 384, 4 * 768 + 4 * 384 + 4 * 192]

    for q in range(4):
        here = other.at[pl.ds(q * colour, colour)]
        copy(here, here, ssem.at[q], rsem.at[q], twin).wait_recv()
        add(part, q * colour, full, c * half + q * colour, other, q * colour, colour)
        offset[q] = q * colour
        axis, kind = STEPS[q][0]
        size = colour // 2
        k = keep(axis, kind)
        go(
            part.at[rows(offset[q] + (1 - k) * size, size)],
            got.at[pl.ds(got_at[0] + q * size, size)],
            ssem.at[4 + q],
            rsem.at[4 + q],
            partner(axis, kind),
        )
        offset[q] = offset[q] + k * size

    for step in range(4):
        size = colour >> (step + 1)
        for q in range(4):
            axis, kind = STEPS[q][step]
            here = got.at[pl.ds(got_at[step] + q * size, size)]
            sem = 4 + 4 * step + q
            copy(here, here, ssem.at[sem], rsem.at[sem], partner(axis, kind)).wait_recv()
            add(part, offset[q], part, offset[q], got, got_at[step] + q * size, size)
            if step < 3:
                axis, kind = STEPS[q][step + 1]
                nxt = size // 2
                k = keep(axis, kind)
                go(
                    part.at[rows(offset[q] + (1 - k) * nxt, nxt)],
                    got.at[pl.ds(got_at[step + 1] + q * nxt, nxt)],
                    ssem.at[sem + 4],
                    rsem.at[sem + 4],
                    partner(axis, kind),
                )
                offset[q] = offset[q] + k * nxt

    last = colour >> 4
    for q in range(4):
        zin[q * last : (q + 1) * last, :] = part[rows(offset[q], last), :]
    piece = 4 * last // zn
    for d in range(1, zn):
        to = lax.rem(z + d, zn)
        go(
            zin.at[rows(to * piece, piece)],
            zgot.at[pl.ds((d - 1) * piece, piece)],
            zs.at[d - 1],
            zr.at[d - 1],
            (to, x * 8 + y * 2 + c),
        )
    run = zin[rows(z * piece, piece), :].astype(jnp.float32)
    for d in range(1, zn):
        here = zgot.at[pl.ds((d - 1) * piece, piece)]
        copy(here, here, zs.at[d - 1], zr.at[d - 1], twin).wait_recv()
        run = run + zgot[(d - 1) * piece : d * piece, :].astype(jnp.float32)
    zout[...] = run.astype(jnp.bfloat16)
    for d in range(1, zn):
        to = lax.rem(z + d, zn)
        go(
            zout,
            zall.at[rows(z * piece, piece)],
            zs.at[zn - 1 + d - 1],
            zr.at[zn - 1 + d - 1],
            (to, x * 8 + y * 2 + c),
        )
    zall[rows(z * piece, piece), :] = zout[...]
    for d in range(1, zn):
        here = zall.at[pl.ds(0, piece)]
        copy(here, here, zs.at[0], zr.at[zn - 1 + d - 1], twin).wait_recv()
    for step in range(3, -2, -1):
        for q in range(4):
            if step == 3:
                got[rows(got_at[3] + 4 * last + offset[q], last), :] = zall[
                    q * last : (q + 1) * last, :
                ]
            if step >= 0:
                size = colour >> (step + 1)
                if step < 3:
                    axis, kind = STEPS[q][step + 1]
                    sem = 20 + 4 * (step + 1) + q
                    prev = size // 2
                    here = got.at[pl.ds(0, prev)]
                    copy(here, here, ssem.at[sem], rsem.at[sem], twin).wait_recv()
                    offset[q] = offset[q] - keep(axis, kind) * prev
                axis, kind = STEPS[q][step]
                sem = 20 + 4 * step + q
                here = got.at[rows(got_at[3] + 4 * last + offset[q], size)]
                go(here, here, ssem.at[sem], rsem.at[sem], partner(axis, kind))
            else:
                sem = 20 + q
                size = colour // 2
                here = got.at[pl.ds(0, size)]
                copy(here, here, ssem.at[sem], rsem.at[sem], twin).wait_recv()
                base = got_at[3] + 4 * last + q * colour
                here = got.at[pl.ds(base, colour)]
                there = back.at[pl.ds(q * colour, colour)]
                go(here, there, ssem.at[36 + q], rsem.at[36 + q], twin)

    def result(value):
        return (value.astype(jnp.float32) * scale).astype(out_ref.dtype)

    per = n_mat // 2
    base = got_at[3] + 4 * last

    def mine(i, carry):
        for k in range(blocks):
            src = got[rows(base + (i * blocks + k) * width, width), :]
            out_ref[c * per + i, :, k * LANE : (k + 1) * LANE] = result(src)
        return carry

    lax.fori_loop(0, per, mine, 0)
    for q in range(4):
        here = back.at[pl.ds(q * colour, colour)]
        copy(here, here, ssem.at[36 + q], rsem.at[36 + q], twin).wait_recv()

    def theirs(i, carry):
        for k in range(blocks):
            src = back[rows((i * blocks + k) * width, width), :]
            out_ref[(1 - c) * per + i, :, k * LANE : (k + 1) * LANE] = result(src)
        return carry

    lax.fori_loop(0, per, theirs, 0)
    for move in sends:
        move.wait_send()


def total_over_all(grads, scale):
    n_mat, width, _ = grads.shape
    total = n_mat * width * width // LANE
    half = total // 2
    dma = pltpu.SemaphoreType.DMA
    bf = jnp.bfloat16

    def kernel(*refs):
        sum_kernel(scale, *refs)

    return pl.pallas_call(
        kernel,
        out_shape=jax.ShapeDtypeStruct(grads.shape, bf),
        in_specs=[pl.BlockSpec(memory_space=pltpu.VMEM)],
        out_specs=pl.BlockSpec(memory_space=pltpu.VMEM),
        scratch_shapes=[
            pltpu.VMEM((total, LANE), bf),
            pltpu.VMEM((half, LANE), bf),
            pltpu.VMEM((half, LANE), bf),
            pltpu.VMEM((half * 15 // 16 + half, LANE), bf),
            pltpu.VMEM((half, LANE), bf),
            pltpu.VMEM((half // 16, LANE), bf),
            pltpu.VMEM((half // 128, LANE), bf),
            pltpu.VMEM((half // 128 * 7, LANE), bf),
            pltpu.VMEM((half // 16, LANE), bf),
            dma((40,)),
            dma((40,)),
            dma((14,)),
            dma((14,)),
        ],
        compiler_params=pltpu.CompilerParams(
            collective_id=0, has_side_effects=True, vmem_limit_bytes=60 * 1024 * 1024
        ),
        name="sum_over_all",
    )(grads)


def per_device(
    features, cotangent, self_weight, neigh_weight, block_val, block_col, send_idx, send_count
):
    outer = lax.axis_size("gx")
    inner = lax.axis_size("gy")
    devices = outer * inner
    node_rows, width = features.shape
    tile = block_val.shape[2]
    layers = self_weight.shape[0]
    slots = send_idx.shape[2]
    halo_rows = devices * slots
    ext_tiles = (node_rows + halo_rows) // tile
    scale = 1.0 / math.sqrt(node_rows * devices)
    bf, f32 = jnp.bfloat16, jnp.float32
    row_ids = send_idx.reshape(-1)
    live = (jnp.arange(slots, dtype=jnp.int32)[None, :] < send_count.reshape(-1)[:, None]).reshape(
        -1, 1
    )
    pick = ((row_ids[:, None] == jnp.arange(node_rows, dtype=jnp.int32)[None, :]) & live).astype(bf)
    where = (block_col[:, :, None] == jnp.arange(ext_tiles, dtype=jnp.int32)).astype(f32)
    dense = jnp.sum(
        where[:, :, None, :, None] * block_val.astype(f32)[:, :, :, None, :], axis=1
    ).reshape(node_rows, ext_tiles * tile).astype(bf)
    near, far = dense[:, :node_rows], dense[:, node_rows:]
    transposed = (((0,), (0,)), ((), ()))
    against = (((1,), (1,)), ((), ()))

    def dot(a, b, dims=(((1,), (0,)), ((), ()))):
        return lax.dot_general(a, b, dims, preferred_element_type=f32)

    def exchange(array):
        tiles = array.reshape(devices, slots, width)
        tiles = lax.all_to_all(tiles, ("gx", "gy"), split_axis=0, concat_axis=0, tiled=True)
        return tiles.reshape(halo_rows, width)

    hiddens, aggregates, preacts = [features], [], []
    hidden = features
    for layer_at in range(layers):
        arrived = exchange(dot(pick, hidden).astype(bf))
        aggregate = (dot(near, hidden) + dot(far, arrived)).astype(bf)
        preact = dot(hidden, self_weight[layer_at]) + dot(aggregate, neigh_weight[layer_at])
        aggregates.append(aggregate)
        preacts.append(preact)
        if layer_at < layers - 1:
            hidden = jax.nn.silu(preact).astype(bf)
            hiddens.append(hidden)
    terms = [None] * (2 * layers)
    grad = cotangent
    for layer_at in reversed(range(layers)):
        preact = preacts[layer_at]
        sigma = jax.nn.sigmoid(preact)
        delta = (grad.astype(f32) * sigma * (1.0 + preact * (1.0 - sigma))).astype(bf)
        terms[layer_at] = dot(hiddens[layer_at], delta, transposed).astype(bf)
        terms[layers + layer_at] = dot(aggregates[layer_at], delta, transposed).astype(bf)
        upstream = dot(delta, neigh_weight[layer_at], against).astype(bf)
        arrived = exchange(dot(far, upstream, transposed).astype(bf))
        own = dot(delta, self_weight[layer_at], against) + dot(near, upstream, transposed)
        grad = (own + dot(pick, arrived, transposed)).astype(bf)
    sums = total_over_all(jnp.stack(terms), scale)
    return (sums[:layers], sums[layers:], grad)


def solution(mesh):
    return jax.shard_map(
        per_device,
        mesh=mesh,
        in_specs=(
            P(("gx", "gy"), None),
            P(("gx", "gy"), None),
            P(),
            P(),
            P(("gx", "gy"), None, None, None),
            P(("gx", "gy"), None),
            P(("gx", "gy"), None, None),
            P(("gx", "gy"), None),
        ),
        out_specs=(P(), P(), P(("gx", "gy"), None)),
        check_vma=False,
    )
```

```python
import math

import jax
import jax.numpy as jnp
from jax import lax
from jax.experimental import pallas as pl
from jax.experimental.pallas import tpu as pltpu
from jax.sharding import PartitionSpec as P

MESH = pl.DeviceIdType.MESH
LANE = 128
BF, F32 = jnp.bfloat16, jnp.float32
ROWS = (((1,), (0,)), ((), ()))
TRANSPOSED = (((0,), (0,)), ((), ()))
AGAINST = (((1,), (1,)), ((), ()))


def dot(a, b, dims=ROWS):
    return lax.dot_general(a, b, dims, preferred_element_type=F32)


def place():
    z, g = lax.axis_index("gx"), lax.axis_index("gy")
    x, y, c = g // 8, lax.rem(g // 2, 4), lax.rem(g, 2)
    return z, g, x, y, c


def flip(p, kind):
    return p + 1 - 2 * lax.rem(p, 2) if kind == 0 else 3 - p


def kept(p, kind):
    return lax.rem((p + 1) // 2, 2) if kind == 0 else p // 2


def rows(start, size):
    return pl.ds(pl.multiple_of(start, 16), size)


def copy(src, dst, s, r, peer):
    return pltpu.make_async_remote_copy(
        src_ref=src, dst_ref=dst, send_sem=s, recv_sem=r, device_id=peer, device_id_type=MESH
    )


STEPS = (
    (("x", 0), ("x", 1), ("y", 0), ("y", 1)),
    (("x", 1), ("x", 0), ("y", 1), ("y", 0)),
    (("y", 0), ("y", 1), ("x", 0), ("x", 1)),
    (("y", 1), ("y", 0), ("x", 1), ("x", 0)),
)
ZN, GN = 8, 32


def sum_stages(layer, scale, outs, bufs, sems, sends):
    z, g, x, y, c = place()
    full, part, other, got, gath, back, zin, zout, zgot, zall = (b.at[layer] for b in bufs)
    ssem, rsem, zs, zr = (s.at[layer] for s in sems)
    half = part.shape[0]
    colour = half // 4

    def at(x_, y_, c_):
        return (z, x_ * 8 + y_ * 2 + c_)

    def partner(axis, kind):
        return at(flip(x, kind), y, c) if axis == "x" else at(x, flip(y, kind), c)

    def keep(axis, kind):
        return kept(x if axis == "x" else y, kind)

    twin = at(x, y, 1 - c)

    def go(*args):
        move = copy(*args)
        move.start()
        sends.append(move)

    def arrive(ref, start, size, sem):
        here = ref.at[pl.ds(start, size)]
        copy(here, here, zs.at[0], sem, twin).wait_recv()

    def add(dst, base, a, a_base, b, b_base, size):
        s = a[rows(a_base, size), :].astype(F32) + b[pl.ds(b_base, size), :].astype(F32)
        dst[rows(base, size), :] = s.astype(BF)

    offset = [q * colour for q in range(4)]
    got_at = [0, 2 * colour, 3 * colour, 3 * colour + colour // 2]

    def halve(q, step):
        axis, kind = STEPS[q][step]
        size = colour >> (step + 1)
        k = keep(axis, kind)
        go(
            part.at[rows(offset[q] + (1 - k) * size, size)],
            got.at[pl.ds(got_at[step] + q * size, size)],
            ssem.at[4 + 4 * step + q],
            rsem.at[4 + 4 * step + q],
            partner(axis, kind),
        )
        offset[q] = offset[q] + k * size

    for q in range(4):
        src = full.at[rows((1 - c) * half + q * colour, colour)]
        go(src, other.at[pl.ds(q * colour, colour)], ssem.at[q], rsem.at[q], twin)
    yield
    for q in range(4):
        arrive(other, q * colour, colour, rsem.at[q])
        add(part, q * colour, full, c * half + q * colour, other, q * colour, colour)
        halve(q, 0)
    yield
    for step in range(4):
        size = colour >> (step + 1)
        for q in range(4):
            base = got_at[step] + q * size
            arrive(got, base, size, rsem.at[4 + 4 * step + q])
            add(part, offset[q], part, offset[q], got, base, size)
            if step < 3:
                halve(q, step + 1)
        if step < 3:
            yield
    last = colour >> 4
    for q in range(4):
        zin[q * last : (q + 1) * last, :] = part[rows(offset[q], last), :]
    piece = 4 * last // ZN
    for d in range(1, ZN):
        to = lax.rem(z + d, ZN)
        go(
            zin.at[rows(to * piece, piece)],
            zgot.at[pl.ds((d - 1) * piece, piece)],
            zs.at[d - 1],
            zr.at[d - 1],
            (to, g),
        )
    yield
    run = zin[rows(z * piece, piece), :].astype(F32)
    for d in range(1, ZN):
        arrive(zgot, (d - 1) * piece, piece, zr.at[d - 1])
        run = run + zgot[(d - 1) * piece : d * piece, :].astype(F32)
    zout[...] = run.astype(BF)
    for d in range(1, ZN):
        to = lax.rem(z + d, ZN)
        go(zout, zall.at[rows(z * piece, piece)], zs.at[6 + d], zr.at[6 + d], (to, g))
    zall[rows(z * piece, piece), :] = zout[...]
    yield
    for d in range(1, ZN):
        arrive(zall, 0, piece, zr.at[6 + d])
    for step in range(3, -1, -1):
        size = colour >> (step + 1)
        for q in range(4):
            if step == 3:
                gath[rows(offset[q], last), :] = zall[q * last : (q + 1) * last, :]
            else:
                axis, kind = STEPS[q][step + 1]
                arrive(gath, 0, size // 2, rsem.at[20 + 4 * (step + 1) + q])
                offset[q] = offset[q] - keep(axis, kind) * (size // 2)
            axis, kind = STEPS[q][step]
            sem = 20 + 4 * step + q
            here = gath.at[rows(offset[q], size)]
            go(here, here, ssem.at[sem], rsem.at[sem], partner(axis, kind))
        yield
    for q in range(4):
        arrive(gath, 0, colour // 2, rsem.at[20 + q])
        here = pl.ds(q * colour, colour)
        go(gath.at[here], back.at[here], ssem.at[36 + q], rsem.at[36 + q], twin)
    yield
    for q in range(4):
        arrive(back, q * colour, colour, rsem.at[36 + q])
        here = pl.ds(q * colour, colour)
        mine = (gath[here, :].astype(F32) * scale).astype(BF)
        theirs = (back[here, :].astype(F32) * scale).astype(BF)
        lanes = pl.ds(q * LANE, LANE)
        first = c == 0
        outs[0][layer, :, lanes] = jnp.where(first, mine, theirs)
        outs[1][layer, :, lanes] = jnp.where(first, theirs, mine)
    yield


def step_kernel(
    scale,
    col_ref,
    idx_ref,
    val_ref,
    feat_ref,
    cot_ref,
    ws_ref,
    wn_ref,
    self_ref,
    neigh_ref,
    in_ref,
    h,
    agg,
    pre,
    base,
    aggn,
    near,
    far,
    far_t,
    pick,
    pick_t,
    perm,
    out1,
    got1,
    out2,
    got2,
    full,
    part,
    other,
    got,
    gath,
    back,
    zin,
    zout,
    zgot,
    zall,
    s1,
    r1,
    s2,
    r2,
    ssem,
    rsem,
    zs,
    zr,
):
    z, g, x, y, c = place()
    node_rows, width = feat_ref.shape
    layers = ws_ref.shape[0]
    halo = idx_ref.shape[1]
    tile = val_ref.shape[2]
    wide = width // 2
    zrow, grow = halo // ZN, halo // GN

    def gpeer(d):
        px = lax.rem(x + d // 8, 4)
        py = lax.rem(y + lax.rem(d // 2, 4), 4)
        pc = lax.rem(c + lax.rem(d, 2), 2)
        return px * 8 + py * 2 + pc

    bar = pltpu.get_barrier_semaphore()
    for d in range(1, ZN):
        pl.semaphore_signal(
            bar, inc=1, device_id=(lax.rem(z + d, ZN), g), device_id_type=MESH
        )

    def greet(d, carry):
        pl.semaphore_signal(bar, inc=1, device_id=(z, gpeer(d)), device_id_type=MESH)
        return carry

    lax.fori_loop(1, GN, greet, 0)

    node = lax.broadcasted_iota(jnp.int32, (node_rows, halo), 0)
    pick_t[0] = (node == idx_ref[...]).astype(F32).astype(BF)
    pick[0] = pick_t[0].T
    i = lax.broadcasted_iota(jnp.int32, (halo, halo), 0)
    j = lax.broadcasted_iota(jnp.int32, (halo, halo), 1)
    perm[0] = (j == ((i >> 1) & 7) * 64 + (i >> 4) * 2 + (i & 1)).astype(F32).astype(BF)
    perm[1] = (j == ((i >> 1) & 31) * 16 + (i >> 6) * 2 + (i & 1)).astype(F32).astype(BF)
    pick[1] = dot(perm[0], pick[0]).astype(BF)
    tiles_near = node_rows // tile
    for r in range(col_ref.shape[0]):
        for t in range(tiles_near + halo // tile):
            block = jnp.zeros((tile, tile), F32)
            for b in range(col_ref.shape[1]):
                on = (col_ref[r, b] == t).astype(F32)
                block = block + val_ref[r, b].astype(F32) * on
            at = slice(r * tile, (r + 1) * tile)
            if t < tiles_near:
                near[at, t * tile : (t + 1) * tile] = block.astype(BF)
            else:
                k = t - tiles_near
                far[0, at, k * tile : (k + 1) * tile] = block.astype(BF)
    h[0] = feat_ref[...]
    pl.semaphore_wait(bar, ZN - 1 + GN - 1)

    def send_z(src, dst, s, r):
        for d in (4, 3, 5, 2, 6, 1, 7):
            to = lax.rem(z + d, ZN)
            copy(
                src.at[rows(to * zrow, zrow)], dst.at[rows(z * zrow, zrow)], s, r, (to, g)
            ).start()
        dst[rows(z * zrow, zrow), :] = src[rows(z * zrow, zrow), :]

    def send_g(src, dst, s, r):
        def body(d, carry):
            to = gpeer(d)
            copy(
                src.at[rows(to * grow, grow)], dst.at[rows(g * grow, grow)], s, r, (z, to)
            ).start()
            return carry

        lax.fori_loop(1, GN, body, 0)
        dst[rows(g * grow, grow), :] = src[rows(g * grow, grow), :]

    def wait_z(dst, r):
        here = dst.at[pl.ds(0, halo - zrow)]
        copy(here, here, r, r, (z, g)).wait_recv()

    def wait_g(dst, r):
        here = dst.at[pl.ds(0, halo - grow)]
        copy(here, here, r, r, (z, g)).wait_recv()

    def start(t, left, right):
        out1[t, 0] = left()
        send_z(out1.at[t, 0], got1.at[t, 0], s1.at[t, 0], r1.at[t, 0])
        out1[t, 1] = right()
        send_g(out1.at[t, 1], got1.at[t, 1], s1.at[t, 1], r1.at[t, 1])

    def turn_right(t):
        wait_g(got1.at[t, 1], r1.at[t, 1])
        out2[t, 1] = dot(perm[1], got1[t, 1]).astype(BF)
        send_z(out2.at[t, 1], got2.at[t, 1], s2.at[t, 1], r2.at[t, 1])

    def turn_left(t):
        wait_z(got1.at[t, 0], r1.at[t, 0])
        out2[t, 0] = dot(perm[0], got1[t, 0]).astype(BF)
        send_g(out2.at[t, 0], got2.at[t, 0], s2.at[t, 0], r2.at[t, 0])

    def forward(t, carry):
        start(
            t,
            lambda: dot(pick[0], h[t, :, :wide]).astype(BF),
            lambda: dot(pick[1], h[t, :, wide:]).astype(BF),
        )
        base[...] = dot(h[t], ws_ref[t])
        aggn[...] = dot(near[...], h[t])
        far[1] = dot(far[0], perm[1]).astype(BF)
        turn_right(t)
        turn_left(t)
        wait_g(got2.at[t, 0], r2.at[t, 0])
        agg[t, :, :wide] = (aggn[:, :wide] + dot(far[1], got2[t, 0])).astype(BF)
        wait_z(got2.at[t, 1], r2.at[t, 1])
        agg[t, :, wide:] = (aggn[:, wide:] + dot(far[0], got2[t, 1])).astype(BF)
        v = base[...] + dot(agg[t], wn_ref[t])
        pre[t] = v
        h[t + 1] = (v * jax.nn.sigmoid(v)).astype(BF)
        return carry

    lax.fori_loop(0, layers, forward, 0)
    for k in range(2):
        far_t[k] = far[k].T
    pick_t[1] = pick[1].T

    outs = (self_ref, neigh_ref)
    bufs = (full, part, other, got, gath, back, zin, zout, zgot, zall)
    sems = (ssem, rsem, zs, zr)
    sends, running = [], []

    def advance():
        for r in running:
            next(r)

    grad = cot_ref
    for at in range(layers - 1, -1, -1):
        t = 2 * layers - 1 - at
        v = pre[at]
        sigma = jax.nn.sigmoid(v)
        delta = (grad[...].astype(F32) * sigma * (1.0 + v * (1.0 - sigma))).astype(BF)
        up = dot(delta, wn_ref[at], AGAINST).astype(BF)
        start(
            t,
            lambda: dot(far_t[0], up[:, :wide]).astype(BF),
            lambda: dot(far_t[1], up[:, wide:]).astype(BF),
        )
        for m, left in enumerate((h, agg)):
            for k in range(2):
                term = dot(left[at], delta[:, k * wide : (k + 1) * wide], TRANSPOSED).astype(BF)
                for n in range(wide // LANE):
                    full[at, pl.ds((m * 4 + k * 2 + n) * width, width), :] = term[
                        :, n * LANE : (n + 1) * LANE
                    ]
        running.append(sum_stages(at, scale, outs, bufs, sems, sends))
        advance()
        base[...] = dot(delta, ws_ref[at], AGAINST) + dot(near[...], up, TRANSPOSED)
        turn_right(t)
        advance()
        turn_left(t)
        advance()
        wait_g(got2.at[t, 0], r2.at[t, 0])
        in_ref[:, :wide] = (base[:, :wide] + dot(pick_t[1], got2[t, 0])).astype(BF)
        wait_z(got2.at[t, 1], r2.at[t, 1])
        in_ref[:, wide:] = (base[:, wide:] + dot(pick_t[0], got2[t, 1])).astype(BF)
        grad = in_ref
    for run in running:
        pass
    alive = list(running)
    while alive:
        for run in list(alive):
            if next(run, "done") == "done":
                alive.remove(run)
    for move in sends:
        move.wait_send()

    def drain(t, carry):
        for k, (first, second) in enumerate(((zrow, grow), (grow, zrow))):
            for ref, sem, own in ((out1, s1, first), (out2, s2, second)):
                here = ref.at[t, k, pl.ds(0, halo - own)]
                copy(here, here, sem.at[t, k], sem.at[t, k], (z, g)).wait_send()
        return carry

    lax.fori_loop(0, 2 * layers, drain, 0)


def whole_step(col, idx, val, feat, cot, ws, wn, scale):
    layers, width, _ = ws.shape
    node_rows, halo = feat.shape[0], idx.shape[1]
    steps = 2 * layers
    total = 2 * width * width // LANE
    half = total // 2
    dma = pltpu.SemaphoreType.DMA
    vm = pltpu.VMEM

    def kernel(*refs):
        step_kernel(scale, *refs)

    grads = jax.ShapeDtypeStruct(ws.shape, BF)
    flow = vm((steps, 2, halo, width // 2), BF)
    return pl.pallas_call(
        kernel,
        out_shape=(grads, grads, jax.ShapeDtypeStruct(feat.shape, BF)),
        in_specs=[pl.BlockSpec(memory_space=pltpu.SMEM)]
        + [pl.BlockSpec(memory_space=pltpu.VMEM)] * 6,
        out_specs=[pl.BlockSpec(memory_space=pltpu.VMEM)] * 3,
        scratch_shapes=[
            vm((layers + 1, node_rows, width), BF),
            vm((layers, node_rows, width), BF),
            vm((layers, node_rows, width), F32),
            vm((node_rows, width), F32),
            vm((node_rows, width), F32),
            vm((node_rows, node_rows), BF),
            vm((2, node_rows, halo), BF),
            vm((2, halo, node_rows), BF),
            vm((2, halo, node_rows), BF),
            vm((2, node_rows, halo), BF),
            vm((2, halo, halo), BF),
            flow,
            flow,
            flow,
            flow,
            vm((layers, total, LANE), BF),
            vm((layers, half, LANE), BF),
            vm((layers, half, LANE), BF),
            vm((layers, half * 15 // 16, LANE), BF),
            vm((layers, half, LANE), BF),
            vm((layers, half, LANE), BF),
            vm((layers, half // 16, LANE), BF),
            vm((layers, half // 128, LANE), BF),
            vm((layers, half // 128 * 7, LANE), BF),
            vm((layers, half // 16, LANE), BF),
            dma((steps, 2)),
            dma((steps, 2)),
            dma((steps, 2)),
            dma((steps, 2)),
            dma((layers, 40)),
            dma((layers, 40)),
            dma((layers, 14)),
            dma((layers, 14)),
        ],
        compiler_params=pltpu.CompilerParams(
            collective_id=0, has_side_effects=True, vmem_limit_bytes=60 * 1024 * 1024
        ),
        name="whole_step",
    )(col, idx, val, feat, cot, ws, wn)


def per_device(
    features, cotangent, self_weight, neigh_weight, block_val, block_col, send_idx, send_count
):
    devices = lax.axis_size("gx") * lax.axis_size("gy")
    slots = send_idx.shape[2]
    scale = 1.0 / math.sqrt(features.shape[0] * devices)
    live = jnp.arange(slots, dtype=jnp.int32)[None, None, :] < send_count[:, :, None]
    idx = jnp.where(live, send_idx, -1).reshape(1, devices * slots)
    return whole_step(
        block_col, idx, block_val, features, cotangent, self_weight, neigh_weight, scale
    )


def solution(mesh):
    return jax.shard_map(
        per_device,
        mesh=mesh,
        in_specs=(
            P(("gx", "gy"), None),
            P(("gx", "gy"), None),
            P(),
            P(),
            P(("gx", "gy"), None, None, None),
            P(("gx", "gy"), None),
            P(("gx", "gy"), None, None),
            P(("gx", "gy"), None),
        ),
        out_specs=(P(), P(), P(("gx", "gy"), None)),
        check_vma=False,
    )
```

```python
import math

import jax
import jax.numpy as jnp
from jax import lax
from jax.experimental import pallas as pl
from jax.experimental.pallas import tpu as pltpu
from jax.sharding import PartitionSpec as P

MESH = pl.DeviceIdType.MESH
LANE = 128
BF, F32 = jnp.bfloat16, jnp.float32
ROWS = (((1,), (0,)), ((), ()))
TRANSPOSED = (((0,), (0,)), ((), ()))
AGAINST = (((1,), (1,)), ((), ()))


def dot(a, b, dims=ROWS):
    return lax.dot_general(a, b, dims, preferred_element_type=F32)


def place():
    z, g = lax.axis_index("gx"), lax.axis_index("gy")
    x, y, c = g // 8, lax.rem(g // 2, 4), lax.rem(g, 2)
    return z, g, x, y, c


def rows(start, size):
    return pl.ds(pl.multiple_of(start, 16), size)


def copy(src, dst, s, r, peer):
    return pltpu.make_async_remote_copy(
        src_ref=src, dst_ref=dst, send_sem=s, recv_sem=r, device_id=peer, device_id_type=MESH
    )


ZN, GN = 8, 32


def sum_stages(layer, outs, bufs, sems, sends):
    z, g, x, y, c = place()
    full, part, other, got, gath, back, zin, zout, zgot, zall = (b.at[layer] for b in bufs)
    ssem, rsem, zs, zr = (s.at[layer] for s in sems)
    half = part.shape[0]
    colour = half // 2
    first, second = colour // 4, colour // 16
    twin = (z, x * 8 + y * 2 + 1 - c)
    axes = ((x, 8, y * 2 + c), (y, 2, x * 8 + c))

    def go(*args):
        move = copy(*args)
        move.start()
        sends.append(move)

    def arrive(ref, start, size, sem):
        here = ref.at[pl.ds(start, size)]
        copy(here, here, zs.at[0], sem, twin).wait_recv()

    def ring(axis, d):
        p, stride, rest = axes[axis]
        to = lax.rem(p + d, 4)
        return to, (z, to * stride + rest)

    def scatter(q, axis, base, size, land, sem):
        for d in range(1, 4):
            to, peer = ring(axis, d)
            go(
                part.at[rows(base + to * size, size)],
                got.at[pl.ds(land + (d - 1) * size, size)],
                ssem.at[sem + d - 1],
                rsem.at[sem + d - 1],
                peer,
            )

    def collect(base, size, land, sem):
        run = part[rows(base, size), :].astype(F32)
        for d in range(3):
            arrive(got, land + d * size, size, rsem.at[sem + d])
            run = run + got[land + d * size : land + (d + 1) * size, :].astype(F32)
        return run.astype(BF)

    def spread(axis, base, size, sem):
        for d in range(1, 4):
            here = gath.at[rows(base, size)]
            go(here, here, ssem.at[sem + d - 1], rsem.at[sem + d - 1], ring(axis, d)[1])

    for q in range(2):
        src = full.at[rows((1 - c) * half + q * colour, colour)]
        go(src, other.at[pl.ds(q * colour, colour)], ssem.at[q], rsem.at[q], twin)
    yield
    outer, inner = [], []
    for q in range(2):
        arrive(other, q * colour, colour, rsem.at[q])
        for k in range(4):
            at = q * colour + k * first
            s = full[rows(c * half + at, first), :].astype(F32)
            part[at : at + first, :] = (s + other[at : at + first, :].astype(F32)).astype(BF)
        scatter(q, q, q * colour, first, q * 3 * first, 2 + 3 * q)
        outer.append(q * colour + axes[q][0] * first)
        inner.append(outer[q] + axes[1 - q][0] * second)
    yield
    for q in range(2):
        part[rows(outer[q], first), :] = collect(outer[q], first, q * 3 * first, 2 + 3 * q)
        scatter(q, 1 - q, outer[q], second, 6 * first + q * 3 * second, 8 + 3 * q)
    yield
    for q in range(2):
        zin[q * second : (q + 1) * second, :] = collect(
            inner[q], second, 6 * first + q * 3 * second, 8 + 3 * q
        )
    piece = 2 * second // ZN
    for d in range(1, ZN):
        to = lax.rem(z + d, ZN)
        go(
            zin.at[rows(to * piece, piece)],
            zgot.at[pl.ds((d - 1) * piece, piece)],
            zs.at[d - 1],
            zr.at[d - 1],
            (to, g),
        )
    yield
    run = zin[rows(z * piece, piece), :].astype(F32)
    for d in range(1, ZN):
        arrive(zgot, (d - 1) * piece, piece, zr.at[d - 1])
        run = run + zgot[(d - 1) * piece : d * piece, :].astype(F32)
    zout[...] = run.astype(BF)
    for d in range(1, ZN):
        to = lax.rem(z + d, ZN)
        go(zout, zall.at[rows(z * piece, piece)], zs.at[6 + d], zr.at[6 + d], (to, g))
    zall[rows(z * piece, piece), :] = zout[...]
    yield
    for d in range(1, ZN):
        arrive(zall, 0, piece, zr.at[6 + d])
    for q in range(2):
        gath[rows(inner[q], second), :] = zall[q * second : (q + 1) * second, :]
        spread(1 - q, inner[q], second, 14 + 3 * q)
    yield
    for q in range(2):
        for d in range(3):
            arrive(gath, 0, second, rsem.at[14 + 3 * q + d])
        spread(q, outer[q], first, 20 + 3 * q)
    yield
    for q in range(2):
        for d in range(3):
            arrive(gath, 0, first, rsem.at[20 + 3 * q + d])
        here = pl.ds(q * colour, colour)
        go(gath.at[here], back.at[here], ssem.at[26 + q], rsem.at[26 + q], twin)
    yield
    width = outs[0].shape[1]
    for k in range(half // width):
        if k % 2 == 0:
            arrive(back, (k // 2) * colour, colour, rsem.at[26 + k // 2])
        here = pl.ds(k * width, width)
        mine, theirs = gath[here, :], back[here, :]
        lanes = pl.ds(k * LANE, LANE)
        even = c == 0
        outs[0][layer, :, lanes] = jnp.where(even, mine, theirs)
        outs[1][layer, :, lanes] = jnp.where(even, theirs, mine)
    yield


def step_kernel(
    col_in,
    idx_in,
    cnt_in,
    val_in,
    feat_in,
    cot_in,
    ws_in,
    wn_in,
    self_ref,
    neigh_ref,
    in_ref,
    col_ref,
    idx_ref,
    cnt_ref,
    val_ref,
    cot_ref,
    ws_ref,
    wn_ref,
    h,
    agg,
    pre,
    base,
    aggn,
    near,
    far,
    far_t,
    pick,
    pick_t,
    perm,
    out1,
    got1,
    out2,
    got2,
    full,
    part,
    other,
    got,
    gath,
    back,
    zin,
    zout,
    zgot,
    zall,
    s1,
    r1,
    s2,
    r2,
    ssem,
    rsem,
    zs,
    zr,
    load,
):
    z, g, x, y, c = place()
    node_rows, width = feat_in.shape
    layers = ws_in.shape[0]
    devices = idx_in.shape[1]
    halo = devices * idx_in.shape[0]
    tile = val_ref.shape[2]
    wide = width // 2
    zrow, grow = halo // ZN, halo // GN

    def gpeer(d):
        px = lax.rem(x + d // 8, 4)
        py = lax.rem(y + lax.rem(d // 2, 4), 4)
        pc = lax.rem(c + lax.rem(d, 2), 2)
        return px * 8 + py * 2 + pc

    loads = [
        pltpu.make_async_copy(src, dst, load.at[k])
        for k, (src, dst) in enumerate(
            (
                (idx_in, idx_ref),
                (cnt_in, cnt_ref),
                (feat_in, h.at[0]),
                (val_in, val_ref),
                (col_in, col_ref),
                (ws_in, ws_ref),
                (wn_in, wn_ref),
                (cot_in, cot_ref),
            )
        )
    ]
    for move in loads:
        move.start()
    bar = pltpu.get_barrier_semaphore()
    for d in range(1, ZN):
        pl.semaphore_signal(
            bar, inc=1, device_id=(lax.rem(z + d, ZN), g), device_id_type=MESH
        )

    def greet(d, carry):
        pl.semaphore_signal(bar, inc=1, device_id=(z, gpeer(d)), device_id_type=MESH)
        return carry

    lax.fori_loop(1, GN, greet, 0)

    i = lax.broadcasted_iota(jnp.int32, (halo, halo), 0)
    j = lax.broadcasted_iota(jnp.int32, (halo, halo), 1)

    def one_hot(target):
        return (j == target).astype(F32).astype(BF)

    node = lax.broadcasted_iota(jnp.int32, (node_rows, devices), 0)
    loads[0].wait()
    loads[1].wait()
    for s in range(halo // devices):
        row = jnp.where(s < cnt_ref[...], idx_ref[s : s + 1, :], -1)
        pick_t[0, :, s * devices : (s + 1) * devices] = (node == row).astype(F32).astype(BF)
    pick[0] = pick_t[0].T
    by_slot = pick[0]
    pick[1] = dot(one_hot((i & 1) * 256 + ((i >> 1) & 7) * 32 + (i >> 4)), by_slot).astype(BF)
    pick[0] = dot(one_hot((i & 1) * 256 + (i >> 1)), by_slot).astype(BF)
    loads[2].wait()

    def constants():
        perm[0] = one_hot(((i >> 1) & 7) * 64 + (i >> 4) * 2 + (i & 1))
        perm[1] = one_hot(((i >> 1) & 31) * 16 + (i >> 6) * 2 + (i & 1))
        for move in loads[3:]:
            move.wait()
        tiles_near = node_rows // tile
        for r in range(col_ref.shape[0]):
            for t in range(tiles_near + halo // tile):
                block = jnp.zeros((tile, tile), F32)
                for b in range(col_ref.shape[1]):
                    on = (col_ref[r, b] == t).astype(F32)
                    block = block + val_ref[r, b].astype(F32) * on
                at = slice(r * tile, (r + 1) * tile)
                if t < tiles_near:
                    near[at, t * tile : (t + 1) * tile] = block.astype(BF)
                else:
                    k = t - tiles_near
                    far[0, at, k * tile : (k + 1) * tile] = block.astype(BF)
        far[1] = dot(far[0], perm[1]).astype(BF)

    pl.semaphore_wait(bar, ZN - 1 + GN - 1)

    def send_z(src, dst, s, r):
        for d in (4, 3, 5, 2, 6, 1, 7):
            to = lax.rem(z + d, ZN)
            copy(
                src.at[rows(to * zrow, zrow)], dst.at[rows(z * zrow, zrow)], s, r, (to, g)
            ).start()
        dst[rows(z * zrow, zrow), :] = src[rows(z * zrow, zrow), :]

    def send_g(src, dst, s, r):
        def body(d, carry):
            to = gpeer(d)
            copy(
                src.at[rows(to * grow, grow)], dst.at[rows(g * grow, grow)], s, r, (z, to)
            ).start()
            return carry

        lax.fori_loop(1, GN, body, 0)
        dst[rows(g * grow, grow), :] = src[rows(g * grow, grow), :]

    def wait_z(dst, r):
        here = dst.at[pl.ds(0, halo - zrow)]
        copy(here, here, r, r, (z, g)).wait_recv()

    def wait_g(dst, r):
        here = dst.at[pl.ds(0, halo - grow)]
        copy(here, here, r, r, (z, g)).wait_recv()

    def start(t, left, right):
        out1[t, 1] = right()
        send_g(out1.at[t, 1], got1.at[t, 1], s1.at[t, 1], r1.at[t, 1])
        out1[t, 0] = left()
        send_z(out1.at[t, 0], got1.at[t, 0], s1.at[t, 0], r1.at[t, 0])

    def turn_right(t):
        wait_g(got1.at[t, 1], r1.at[t, 1])
        out2[t, 1] = dot(perm[1], got1[t, 1]).astype(BF)
        send_z(out2.at[t, 1], got2.at[t, 1], s2.at[t, 1], r2.at[t, 1])

    def turn_left(t):
        wait_z(got1.at[t, 0], r1.at[t, 0])
        out2[t, 0] = dot(perm[0], got1[t, 0]).astype(BF)
        send_g(out2.at[t, 0], got2.at[t, 0], s2.at[t, 0], r2.at[t, 0])

    def slope(v):
        sigma = jax.nn.sigmoid(v)
        return sigma * (1.0 + v * (1.0 - sigma))

    def forward(t, between):
        start(
            t,
            lambda: dot(pick[0], h[t, :, :wide]).astype(BF),
            lambda: dot(pick[1], h[t, :, wide:]).astype(BF),
        )
        between()
        base[...] = dot(h[t], ws_ref[t])
        aggn[...] = dot(near[...], h[t])
        turn_right(t)
        turn_left(t)
        wait_g(got2.at[t, 0], r2.at[t, 0])
        agg[t, :, :wide] = (aggn[:, :wide] + dot(far[1], got2[t, 0])).astype(BF)
        base[...] += dot(agg[t, :, :wide], wn_ref[t, :wide, :])
        wait_z(got2.at[t, 1], r2.at[t, 1])
        agg[t, :, wide:] = (aggn[:, wide:] + dot(far[0], got2[t, 1])).astype(BF)
        v = base[...] + dot(agg[t, :, wide:], wn_ref[t, wide:, :])
        pre[t] = v
        h[t + 1] = (v * jax.nn.sigmoid(v)).astype(BF)

    forward(0, constants)

    def later(t, carry):
        def between():
            pre[t - 1] = slope(pre[t - 1])

        forward(t, between)
        return carry

    lax.fori_loop(1, layers, later, 0)
    for k in range(2):
        far_t[k] = far[k].T
        pick_t[k] = pick[k].T

    outs = (self_ref, neigh_ref)
    bufs = (full, part, other, got, gath, back, zin, zout, zgot, zall)
    sems = (ssem, rsem, zs, zr)
    sends, running = [], []

    def advance():
        for run in list(running):
            if next(run, "done") == "done":
                running.remove(run)

    grad = cot_ref
    for at in range(layers - 1, -1, -1):
        t = 2 * layers - 1 - at
        if at == layers - 1:
            pre[at] = slope(pre[at])
        delta = (grad[...].astype(F32) * pre[at]).astype(BF)
        up = dot(delta, wn_ref[at], AGAINST).astype(BF)
        start(
            t,
            lambda: dot(far_t[0], up[:, :wide]).astype(BF),
            lambda: dot(far_t[1], up[:, wide:]).astype(BF),
        )
        for m, left in enumerate((h, agg)):
            for k in range(2):
                term = dot(left[at], delta[:, k * wide : (k + 1) * wide], TRANSPOSED).astype(BF)
                for n in range(wide // LANE):
                    full[at, pl.ds((m * 4 + k * 2 + n) * width, width), :] = term[
                        :, n * LANE : (n + 1) * LANE
                    ]
        running.append(sum_stages(at, outs, bufs, sems, sends))
        advance()
        base[...] = dot(delta, ws_ref[at], AGAINST) + dot(near[...], up, TRANSPOSED)
        advance()
        turn_right(t)
        advance()
        turn_left(t)
        advance()
        wait_g(got2.at[t, 0], r2.at[t, 0])
        in_ref[:, :wide] = (base[:, :wide] + dot(pick_t[1], got2[t, 0])).astype(BF)
        advance()
        wait_z(got2.at[t, 1], r2.at[t, 1])
        in_ref[:, wide:] = (base[:, wide:] + dot(pick_t[0], got2[t, 1])).astype(BF)
        grad = in_ref
    while running:
        advance()
    for move in sends:
        move.wait_send()

    def drain(t, carry):
        for k, (first, second) in enumerate(((zrow, grow), (grow, zrow))):
            for ref, sem, own in ((out1, s1, first), (out2, s2, second)):
                here = ref.at[t, k, pl.ds(0, halo - own)]
                copy(here, here, sem.at[t, k], sem.at[t, k], (z, g)).wait_send()
        return carry

    lax.fori_loop(0, 2 * layers, drain, 0)


def whole_step(col, idx, cnt, val, feat, cot, ws, wn):
    layers, width, _ = ws.shape
    node_rows, halo = feat.shape[0], idx.shape[0] * idx.shape[1]
    steps = 2 * layers
    total = 2 * width * width // LANE
    half = total // 2
    dma = pltpu.SemaphoreType.DMA
    vm = pltpu.VMEM

    grads = jax.ShapeDtypeStruct(ws.shape, BF)
    flow = vm((steps, 2, halo, width // 2), BF)
    return pl.pallas_call(
        step_kernel,
        out_shape=(grads, grads, jax.ShapeDtypeStruct(feat.shape, BF)),
        in_specs=[pl.BlockSpec(memory_space=pltpu.HBM)] * 8,
        out_specs=[pl.BlockSpec(memory_space=pltpu.VMEM)] * 3,
        scratch_shapes=[
            pltpu.SMEM(col.shape, col.dtype),
            vm(idx.shape, idx.dtype),
            vm(cnt.shape, cnt.dtype),
            vm(val.shape, BF),
            vm(cot.shape, BF),
            vm(ws.shape, BF),
            vm(wn.shape, BF),
            vm((layers + 1, node_rows, width), BF),
            vm((layers, node_rows, width), BF),
            vm((layers, node_rows, width), F32),
            vm((node_rows, width), F32),
            vm((node_rows, width), F32),
            vm((node_rows, node_rows), BF),
            vm((2, node_rows, halo), BF),
            vm((2, halo, node_rows), BF),
            vm((2, halo, node_rows), BF),
            vm((2, node_rows, halo), BF),
            vm((2, halo, halo), BF),
            flow,
            flow,
            flow,
            flow,
            vm((layers, total, LANE), BF),
            vm((layers, half, LANE), BF),
            vm((layers, half, LANE), BF),
            vm((layers, half * 15 // 16, LANE), BF),
            vm((layers, half, LANE), BF),
            vm((layers, half, LANE), BF),
            vm((layers, half // 16, LANE), BF),
            vm((layers, half // 128, LANE), BF),
            vm((layers, half // 128 * 7, LANE), BF),
            vm((layers, half // 16, LANE), BF),
            dma((steps, 2)),
            dma((steps, 2)),
            dma((steps, 2)),
            dma((steps, 2)),
            dma((layers, 28)),
            dma((layers, 28)),
            dma((layers, 14)),
            dma((layers, 14)),
            dma((8,)),
        ],
        compiler_params=pltpu.CompilerParams(
            collective_id=0, has_side_effects=True, vmem_limit_bytes=60 * 1024 * 1024
        ),
        name="whole_step",
    )(col, idx, cnt, val, feat, cot, ws, wn)


def per_device(
    features, cotangent, self_weight, neigh_weight, block_val, block_col, send_idx, send_count
):
    devices = lax.axis_size("gx") * lax.axis_size("gy")
    slots = send_idx.shape[2]
    scale = 1.0 / math.sqrt(features.shape[0] * devices)
    self_sum, neigh_sum, grad = whole_step(
        block_col,
        send_idx.reshape(devices, slots).T,
        send_count,
        block_val,
        features,
        cotangent,
        self_weight,
        neigh_weight,
    )

    def scaled(total):
        return (total.astype(F32) * scale).astype(BF)

    return scaled(self_sum), scaled(neigh_sum), grad


def solution(mesh):
    return jax.shard_map(
        per_device,
        mesh=mesh,
        in_specs=(
            P(("gx", "gy"), None),
            P(("gx", "gy"), None),
            P(),
            P(),
            P(("gx", "gy"), None, None, None),
            P(("gx", "gy"), None),
            P(("gx", "gy"), None, None),
            P(("gx", "gy"), None),
        ),
        out_specs=(P(), P(), P(("gx", "gy"), None)),
        check_vma=False,
    )
```

```python
import math

import jax
import jax.numpy as jnp
from jax import lax
from jax.experimental import pallas as pl
from jax.experimental.pallas import tpu as pltpu
from jax.sharding import PartitionSpec as P

MESH = pl.DeviceIdType.MESH
LANE = 128
BF, F32 = jnp.bfloat16, jnp.float32
ROWS = (((1,), (0,)), ((), ()))
TRANSPOSED = (((0,), (0,)), ((), ()))
AGAINST = (((1,), (1,)), ((), ()))


def dot(a, b, dims=ROWS):
    return lax.dot_general(a, b, dims, preferred_element_type=F32)


def place():
    z, g = lax.axis_index("gx"), lax.axis_index("gy")
    x, y, c = g // 8, lax.rem(g // 2, 4), lax.rem(g, 2)
    return z, g, x, y, c


def rows(start, size):
    return pl.ds(pl.multiple_of(start, 16), size)


def copy(src, dst, s, r, peer):
    return pltpu.make_async_remote_copy(
        src_ref=src, dst_ref=dst, send_sem=s, recv_sem=r, device_id=peer, device_id_type=MESH
    )


ZN, GN = 8, 32


def sum_stages(layer, outs, bufs, sems, sends):
    z, g, x, y, c = place()
    full, part, other, got, gath, back, zin, zout, zgot, zall = (b.at[layer] for b in bufs)
    ssem, rsem, zs, zr = (s.at[layer] for s in sems)
    half = part.shape[0]
    colour = half // 2
    first, second = colour // 4, colour // 16
    twin = (z, x * 8 + y * 2 + 1 - c)
    axes = ((x, 8, y * 2 + c), (y, 2, x * 8 + c))

    def go(*args):
        move = copy(*args)
        move.start()
        sends.append(move)

    def arrive(ref, start, size, sem):
        here = ref.at[pl.ds(start, size)]
        copy(here, here, zs.at[0], sem, twin).wait_recv()

    def ring(axis, d):
        p, stride, rest = axes[axis]
        to = lax.rem(p + d, 4)
        return to, (z, to * stride + rest)

    def scatter(q, axis, base, size, land, sem):
        for d in range(1, 4):
            to, peer = ring(axis, d)
            go(
                part.at[rows(base + to * size, size)],
                got.at[pl.ds(land + (d - 1) * size, size)],
                ssem.at[sem + d - 1],
                rsem.at[sem + d - 1],
                peer,
            )

    def collect(base, size, land, sem):
        run = part[rows(base, size), :].astype(F32)
        for d in range(3):
            arrive(got, land + d * size, size, rsem.at[sem + d])
            run = run + got[land + d * size : land + (d + 1) * size, :].astype(F32)
        return run.astype(BF)

    def spread(axis, base, size, sem):
        for d in range(1, 4):
            here = gath.at[rows(base, size)]
            go(here, here, ssem.at[sem + d - 1], rsem.at[sem + d - 1], ring(axis, d)[1])

    for q in range(2):
        src = full.at[rows((1 - c) * half + q * colour, colour)]
        go(src, other.at[pl.ds(q * colour, colour)], ssem.at[q], rsem.at[q], twin)
    yield True
    outer, inner = [], []
    for q in range(2):
        arrive(other, q * colour, colour, rsem.at[q])
        for k in range(4):
            at = q * colour + k * first
            s = full[rows(c * half + at, first), :].astype(F32)
            part[at : at + first, :] = (s + other[at : at + first, :].astype(F32)).astype(BF)
        scatter(q, q, q * colour, first, q * 3 * first, 2 + 3 * q)
        outer.append(q * colour + axes[q][0] * first)
        inner.append(outer[q] + axes[1 - q][0] * second)
    yield False
    for q in range(2):
        part[rows(outer[q], first), :] = collect(outer[q], first, q * 3 * first, 2 + 3 * q)
        scatter(q, 1 - q, outer[q], second, 6 * first + q * 3 * second, 8 + 3 * q)
    yield False
    for q in range(2):
        zin[q * second : (q + 1) * second, :] = collect(
            inner[q], second, 6 * first + q * 3 * second, 8 + 3 * q
        )
    piece = 2 * second // ZN
    for d in range(1, ZN):
        to = lax.rem(z + d, ZN)
        go(
            zin.at[rows(to * piece, piece)],
            zgot.at[pl.ds((d - 1) * piece, piece)],
            zs.at[d - 1],
            zr.at[d - 1],
            (to, g),
        )
    yield False
    run = zin[rows(z * piece, piece), :].astype(F32)
    for d in range(1, ZN):
        arrive(zgot, (d - 1) * piece, piece, zr.at[d - 1])
        run = run + zgot[(d - 1) * piece : d * piece, :].astype(F32)
    zout[...] = run.astype(BF)
    for d in range(1, ZN):
        to = lax.rem(z + d, ZN)
        go(zout, zall.at[rows(z * piece, piece)], zs.at[6 + d], zr.at[6 + d], (to, g))
    zall[rows(z * piece, piece), :] = zout[...]
    yield False
    for d in range(1, ZN):
        arrive(zall, 0, piece, zr.at[6 + d])
    for q in range(2):
        gath[rows(inner[q], second), :] = zall[q * second : (q + 1) * second, :]
        spread(1 - q, inner[q], second, 14 + 3 * q)
    yield True
    for q in range(2):
        for d in range(3):
            arrive(gath, 0, second, rsem.at[14 + 3 * q + d])
        spread(q, outer[q], first, 20 + 3 * q)
    yield False
    for q in range(2):
        for d in range(3):
            arrive(gath, 0, first, rsem.at[20 + 3 * q + d])
        here = pl.ds(q * colour, colour)
        go(gath.at[here], back.at[here], ssem.at[26 + q], rsem.at[26 + q], twin)
    yield False
    width = outs[0].shape[1]
    for k in range(half // width):
        if k % 2 == 0:
            arrive(back, (k // 2) * colour, colour, rsem.at[26 + k // 2])
        here = pl.ds(k * width, width)
        mine, theirs = gath[here, :], back[here, :]
        lanes = pl.ds(k * LANE, LANE)
        even = c == 0
        outs[0][layer, :, lanes] = jnp.where(even, mine, theirs)
        outs[1][layer, :, lanes] = jnp.where(even, theirs, mine)
    yield False


def step_kernel(
    col_in,
    idx_in,
    cnt_in,
    val_in,
    feat_in,
    cot_in,
    ws_in,
    wn_in,
    self_ref,
    neigh_ref,
    in_ref,
    col_ref,
    idx_ref,
    cnt_ref,
    val_ref,
    cot_ref,
    ws_ref,
    wn_ref,
    h,
    agg,
    pre,
    base,
    aggn,
    near,
    far,
    far_t,
    pick,
    pick_t,
    perm,
    out1,
    got1,
    out2,
    got2,
    full,
    part,
    other,
    got,
    gath,
    back,
    zin,
    zout,
    zgot,
    zall,
    s1,
    r1,
    s2,
    r2,
    ssem,
    rsem,
    zs,
    zr,
    load,
):
    z, g, x, y, c = place()
    node_rows, width = feat_in.shape
    layers = ws_in.shape[0]
    devices = idx_in.shape[1]
    halo = devices * idx_in.shape[0]
    tile = val_ref.shape[2]
    wide = width // 2
    zrow, grow = halo // ZN, halo // GN

    def gpeer(d):
        px = lax.rem(x + d // 8, 4)
        py = lax.rem(y + lax.rem(d // 2, 4), 4)
        pc = lax.rem(c + lax.rem(d, 2), 2)
        return px * 8 + py * 2 + pc

    loads = [
        pltpu.make_async_copy(src, dst, load.at[k])
        for k, (src, dst) in enumerate(
            (
                (idx_in, idx_ref),
                (cnt_in, cnt_ref),
                (feat_in, h.at[0]),
                (val_in, val_ref),
                (col_in, col_ref),
                (ws_in, ws_ref),
                (wn_in, wn_ref),
                (cot_in, cot_ref),
            )
        )
    ]
    for move in loads:
        move.start()
    bar = pltpu.get_barrier_semaphore()
    for d in range(1, ZN):
        pl.semaphore_signal(
            bar, inc=1, device_id=(lax.rem(z + d, ZN), g), device_id_type=MESH
        )

    def greet(d, carry):
        pl.semaphore_signal(bar, inc=1, device_id=(z, gpeer(d)), device_id_type=MESH)
        return carry

    lax.fori_loop(1, GN, greet, 0)

    i = lax.broadcasted_iota(jnp.int32, (halo, halo), 0)
    j = lax.broadcasted_iota(jnp.int32, (halo, halo), 1)

    def one_hot(target):
        return (j == target).astype(F32).astype(BF)

    node = lax.broadcasted_iota(jnp.int32, (node_rows, devices), 0)
    loads[0].wait()
    loads[1].wait()
    for s in range(halo // devices):
        row = jnp.where(s < cnt_ref[...], idx_ref[s : s + 1, :], -1)
        pick_t[0, :, s * devices : (s + 1) * devices] = (node == row).astype(F32).astype(BF)
    pick[0] = pick_t[0].T
    by_slot = pick[0]
    pick[1] = dot(one_hot((i & 1) * 256 + ((i >> 1) & 7) * 32 + (i >> 4)), by_slot).astype(BF)
    pick[0] = dot(one_hot((i & 1) * 256 + (i >> 1)), by_slot).astype(BF)
    loads[2].wait()

    def constants():
        perm[0] = one_hot(((i >> 1) & 7) * 64 + (i >> 4) * 2 + (i & 1))
        perm[1] = one_hot(((i >> 1) & 31) * 16 + (i >> 6) * 2 + (i & 1))
        for move in loads[3:]:
            move.wait()
        tiles_near = node_rows // tile
        for r in range(col_ref.shape[0]):
            for t in range(tiles_near + halo // tile):
                block = jnp.zeros((tile, tile), F32)
                for b in range(col_ref.shape[1]):
                    on = (col_ref[r, b] == t).astype(F32)
                    block = block + val_ref[r, b].astype(F32) * on
                at = slice(r * tile, (r + 1) * tile)
                if t < tiles_near:
                    near[at, t * tile : (t + 1) * tile] = block.astype(BF)
                else:
                    k = t - tiles_near
                    far[0, at, k * tile : (k + 1) * tile] = block.astype(BF)
        far[1] = dot(far[0], perm[1]).astype(BF)

    pl.semaphore_wait(bar, ZN - 1 + GN - 1)

    def send_z(src, dst, s, r):
        for d in (4, 3, 5, 2, 6, 1, 7):
            to = lax.rem(z + d, ZN)
            copy(
                src.at[rows(to * zrow, zrow)], dst.at[rows(z * zrow, zrow)], s, r, (to, g)
            ).start()
        dst[rows(z * zrow, zrow), :] = src[rows(z * zrow, zrow), :]

    ys = [lax.rem(y + d, 4) for d in range(4)]
    cs = [c, 1 - c]

    def send_g(src, dst, s, r):
        def part(px, own):
            for dy in (2, 1, 3, 0):
                for dc in (1, 0):
                    if own and dy == 0 and dc == 0:
                        continue
                    to = px * 8 + ys[dy] * 2 + cs[dc]
                    copy(
                        src.at[rows(to * grow, grow)], dst.at[rows(g * grow, grow)], s, r, (z, to)
                    ).start()

        def body(d, carry):
            part(lax.rem(x + d, 4), False)
            return carry

        lax.fori_loop(1, 4, body, 0)
        part(x, True)
        dst[rows(g * grow, grow), :] = src[rows(g * grow, grow), :]

    def wait_z(dst, r):
        here = dst.at[pl.ds(0, halo - zrow)]
        copy(here, here, r, r, (z, g)).wait_recv()

    def wait_g(dst, r):
        here = dst.at[pl.ds(0, halo - grow)]
        copy(here, here, r, r, (z, g)).wait_recv()

    def start(t, left, right):
        out1[t, 0] = left()
        send_z(out1.at[t, 0], got1.at[t, 0], s1.at[t, 0], r1.at[t, 0])
        out1[t, 1] = right()
        send_g(out1.at[t, 1], got1.at[t, 1], s1.at[t, 1], r1.at[t, 1])

    def turn_right(t):
        wait_g(got1.at[t, 1], r1.at[t, 1])
        out2[t, 1] = dot(perm[1], got1[t, 1]).astype(BF)
        send_z(out2.at[t, 1], got2.at[t, 1], s2.at[t, 1], r2.at[t, 1])

    def turn_left(t):
        wait_z(got1.at[t, 0], r1.at[t, 0])
        out2[t, 0] = dot(perm[0], got1[t, 0]).astype(BF)
        send_g(out2.at[t, 0], got2.at[t, 0], s2.at[t, 0], r2.at[t, 0])

    def slope(v):
        sigma = jax.nn.sigmoid(v)
        return sigma * (1.0 + v * (1.0 - sigma))

    def forward(t, between):
        start(
            t,
            lambda: dot(pick[0], h[t, :, :wide]).astype(BF),
            lambda: dot(pick[1], h[t, :, wide:]).astype(BF),
        )
        between()
        base[...] = dot(h[t], ws_ref[t])
        aggn[...] = dot(near[...], h[t])
        turn_right(t)
        turn_left(t)
        wait_g(got2.at[t, 0], r2.at[t, 0])
        agg[t, :, :wide] = (aggn[:, :wide] + dot(far[1], got2[t, 0])).astype(BF)
        base[...] += dot(agg[t, :, :wide], wn_ref[t, :wide, :])
        wait_z(got2.at[t, 1], r2.at[t, 1])
        agg[t, :, wide:] = (aggn[:, wide:] + dot(far[0], got2[t, 1])).astype(BF)
        v = base[...] + dot(agg[t, :, wide:], wn_ref[t, wide:, :])
        pre[t] = v
        h[t + 1] = (v * jax.nn.sigmoid(v)).astype(BF)

    forward(0, constants)

    def later(t, carry):
        def between():
            pre[t - 1] = slope(pre[t - 1])

        forward(t, between)
        return carry

    lax.fori_loop(1, layers, later, 0)
    for k in range(2):
        far_t[k] = far[k].T
        pick_t[k] = pick[k].T

    outs = (self_ref, neigh_ref)
    bufs = (full, part, other, got, gath, back, zin, zout, zgot, zall)
    sems = (ssem, rsem, zs, zr)
    sends, running = [], []

    def advance(much=True, only=None):
        for entry in list(running):
            run, layer, heavy = entry
            if (heavy and not much) or only not in (None, layer):
                continue
            entry[2] = next(run, None)
            if entry[2] is None:
                running.remove(entry)

    grad = cot_ref
    for at in range(layers - 1, -1, -1):
        t = 2 * layers - 1 - at
        if at == layers - 1:
            pre[at] = slope(pre[at])
        delta = (grad[...].astype(F32) * pre[at]).astype(BF)
        up = dot(delta, wn_ref[at], AGAINST).astype(BF)
        start(
            t,
            lambda: dot(far_t[0], up[:, :wide]).astype(BF),
            lambda: dot(far_t[1], up[:, wide:]).astype(BF),
        )
        for m, left in enumerate((h, agg)):
            for k in range(2):
                term = dot(left[at], delta[:, k * wide : (k + 1) * wide], TRANSPOSED).astype(BF)
                for n in range(wide // LANE):
                    full[at, pl.ds((m * 4 + k * 2 + n) * width, width), :] = term[
                        :, n * LANE : (n + 1) * LANE
                    ]
        running.append([sum_stages(at, outs, bufs, sems, sends), at, False])
        advance()
        base[...] = dot(delta, ws_ref[at], AGAINST) + dot(near[...], up, TRANSPOSED)
        if at == 0:
            advance()
        turn_right(t)
        turn_left(t)
        advance(much=False)
        advance(much=False)
        wait_g(got2.at[t, 0], r2.at[t, 0])
        in_ref[:, :wide] = (base[:, :wide] + dot(pick_t[1], got2[t, 0])).astype(BF)
        if at == 0:
            advance(only=0)
        wait_z(got2.at[t, 1], r2.at[t, 1])
        in_ref[:, wide:] = (base[:, wide:] + dot(pick_t[0], got2[t, 1])).astype(BF)
        grad = in_ref
    while running:
        advance()
    for move in sends:
        move.wait_send()

    def drain(t, carry):
        for k, (first, second) in enumerate(((zrow, grow), (grow, zrow))):
            for ref, sem, own in ((out1, s1, first), (out2, s2, second)):
                here = ref.at[t, k, pl.ds(0, halo - own)]
                copy(here, here, sem.at[t, k], sem.at[t, k], (z, g)).wait_send()
        return carry

    lax.fori_loop(0, 2 * layers, drain, 0)


def whole_step(col, idx, cnt, val, feat, cot, ws, wn):
    layers, width, _ = ws.shape
    node_rows, halo = feat.shape[0], idx.shape[0] * idx.shape[1]
    steps = 2 * layers
    total = 2 * width * width // LANE
    half = total // 2
    dma = pltpu.SemaphoreType.DMA
    vm = pltpu.VMEM

    grads = jax.ShapeDtypeStruct(ws.shape, BF)
    flow = vm((steps, 2, halo, width // 2), BF)
    return pl.pallas_call(
        step_kernel,
        out_shape=(grads, grads, jax.ShapeDtypeStruct(feat.shape, BF)),
        in_specs=[pl.BlockSpec(memory_space=pltpu.HBM)] * 8,
        out_specs=[pl.BlockSpec(memory_space=pltpu.VMEM)] * 3,
        scratch_shapes=[
            pltpu.SMEM(col.shape, col.dtype),
            vm(idx.shape, idx.dtype),
            vm(cnt.shape, cnt.dtype),
            vm(val.shape, BF),
            vm(cot.shape, BF),
            vm(ws.shape, BF),
            vm(wn.shape, BF),
            vm((layers + 1, node_rows, width), BF),
            vm((layers, node_rows, width), BF),
            vm((layers, node_rows, width), F32),
            vm((node_rows, width), F32),
            vm((node_rows, width), F32),
            vm((node_rows, node_rows), BF),
            vm((2, node_rows, halo), BF),
            vm((2, halo, node_rows), BF),
            vm((2, halo, node_rows), BF),
            vm((2, node_rows, halo), BF),
            vm((2, halo, halo), BF),
            flow,
            flow,
            flow,
            flow,
            vm((layers, total, LANE), BF),
            vm((layers, half, LANE), BF),
            vm((layers, half, LANE), BF),
            vm((layers, half * 15 // 16, LANE), BF),
            vm((layers, half, LANE), BF),
            vm((layers, half, LANE), BF),
            vm((layers, half // 16, LANE), BF),
            vm((layers, half // 128, LANE), BF),
            vm((layers, half // 128 * 7, LANE), BF),
            vm((layers, half // 16, LANE), BF),
            dma((steps, 2)),
            dma((steps, 2)),
            dma((steps, 2)),
            dma((steps, 2)),
            dma((layers, 28)),
            dma((layers, 28)),
            dma((layers, 14)),
            dma((layers, 14)),
            dma((8,)),
        ],
        compiler_params=pltpu.CompilerParams(
            collective_id=0, has_side_effects=True, vmem_limit_bytes=60 * 1024 * 1024
        ),
        name="whole_step",
    )(col, idx, cnt, val, feat, cot, ws, wn)


def per_device(
    features, cotangent, self_weight, neigh_weight, block_val, block_col, send_idx, send_count
):
    devices = lax.axis_size("gx") * lax.axis_size("gy")
    slots = send_idx.shape[2]
    scale = 1.0 / math.sqrt(features.shape[0] * devices)
    self_sum, neigh_sum, grad = whole_step(
        block_col,
        send_idx.reshape(devices, slots).T,
        send_count,
        block_val,
        features,
        cotangent,
        self_weight,
        neigh_weight,
    )

    def scaled(total):
        return (total.astype(F32) * scale).astype(BF)

    return scaled(self_sum), scaled(neigh_sum), grad


def solution(mesh):
    return jax.shard_map(
        per_device,
        mesh=mesh,
        in_specs=(
            P(("gx", "gy"), None),
            P(("gx", "gy"), None),
            P(),
            P(),
            P(("gx", "gy"), None, None, None),
            P(("gx", "gy"), None),
            P(("gx", "gy"), None, None),
            P(("gx", "gy"), None),
        ),
        out_specs=(P(), P(), P(("gx", "gy"), None)),
        check_vma=False,
    )
```

```python
import math

import jax
import jax.numpy as jnp
from jax import lax
from jax.experimental import pallas as pl
from jax.experimental.pallas import tpu as pltpu
from jax.sharding import PartitionSpec as P

MESH = pl.DeviceIdType.MESH
LANE = 128
BF, F32 = jnp.bfloat16, jnp.float32
ROWS = (((1,), (0,)), ((), ()))
TRANSPOSED = (((0,), (0,)), ((), ()))
AGAINST = (((1,), (1,)), ((), ()))


def dot(a, b, dims=ROWS):
    return lax.dot_general(a, b, dims, preferred_element_type=F32)


def place():
    z, g = lax.axis_index("gx"), lax.axis_index("gy")
    x, y, c = g // 8, lax.rem(g // 2, 4), lax.rem(g, 2)
    return z, g, x, y, c


def rows(start, size):
    return pl.ds(pl.multiple_of(start, 16), size)


def copy(src, dst, s, r, peer):
    return pltpu.make_async_remote_copy(
        src_ref=src, dst_ref=dst, send_sem=s, recv_sem=r, device_id=peer, device_id_type=MESH
    )


ZN, GN = 8, 32


def sum_stages(layer, outs, bufs, sems, sends):
    z, g, x, y, c = place()
    full, part, other, got, gath, back, zin, zout, zgot, zall = (b.at[layer] for b in bufs)
    ssem, rsem, zs, zr = (s.at[layer] for s in sems)
    half = part.shape[0]
    colour = half // 2
    first, second = colour // 4, colour // 16
    twin = (z, x * 8 + y * 2 + 1 - c)
    axes = ((x, 8, y * 2 + c), (y, 2, x * 8 + c))

    def go(*args):
        move = copy(*args)
        move.start()
        sends.append(move)

    def arrive(ref, start, size, sem):
        here = ref.at[pl.ds(start, size)]
        copy(here, here, zs.at[0], sem, twin).wait_recv()

    def ring(axis, d):
        p, stride, rest = axes[axis]
        to = lax.rem(p + d, 4)
        return to, (z, to * stride + rest)

    def scatter(q, axis, base, size, land, sem):
        for d in range(1, 4):
            to, peer = ring(axis, d)
            go(
                part.at[rows(base + to * size, size)],
                got.at[pl.ds(land + (d - 1) * size, size)],
                ssem.at[sem + d - 1],
                rsem.at[sem + d - 1],
                peer,
            )

    def collect(base, size, land, sem):
        run = part[rows(base, size), :].astype(F32)
        for d in range(3):
            arrive(got, land + d * size, size, rsem.at[sem + d])
            run = run + got[land + d * size : land + (d + 1) * size, :].astype(F32)
        return run.astype(BF)

    def spread(axis, base, size, sem):
        for d in range(1, 4):
            here = gath.at[rows(base, size)]
            go(here, here, ssem.at[sem + d - 1], rsem.at[sem + d - 1], ring(axis, d)[1])

    for q in range(2):
        src = full.at[rows((1 - c) * half + q * colour, colour)]
        go(src, other.at[pl.ds(q * colour, colour)], ssem.at[q], rsem.at[q], twin)
    yield True
    outer, inner = [], []
    for q in range(2):
        arrive(other, q * colour, colour, rsem.at[q])
        for k in range(4):
            at = q * colour + k * first
            s = full[rows(c * half + at, first), :].astype(F32)
            part[at : at + first, :] = (s + other[at : at + first, :].astype(F32)).astype(BF)
        scatter(q, q, q * colour, first, q * 3 * first, 2 + 3 * q)
        outer.append(q * colour + axes[q][0] * first)
        inner.append(outer[q] + axes[1 - q][0] * second)
    yield False
    for q in range(2):
        part[rows(outer[q], first), :] = collect(outer[q], first, q * 3 * first, 2 + 3 * q)
        scatter(q, 1 - q, outer[q], second, 6 * first + q * 3 * second, 8 + 3 * q)
    yield False
    for q in range(2):
        zin[q * second : (q + 1) * second, :] = collect(
            inner[q], second, 6 * first + q * 3 * second, 8 + 3 * q
        )
    piece = 2 * second // ZN
    for d in range(1, ZN):
        to = lax.rem(z + d, ZN)
        go(
            zin.at[rows(to * piece, piece)],
            zgot.at[pl.ds((d - 1) * piece, piece)],
            zs.at[d - 1],
            zr.at[d - 1],
            (to, g),
        )
    yield False
    run = zin[rows(z * piece, piece), :].astype(F32)
    for d in range(1, ZN):
        arrive(zgot, (d - 1) * piece, piece, zr.at[d - 1])
        run = run + zgot[(d - 1) * piece : d * piece, :].astype(F32)
    zout[...] = run.astype(BF)
    for d in range(1, ZN):
        to = lax.rem(z + d, ZN)
        go(zout, zall.at[rows(z * piece, piece)], zs.at[6 + d], zr.at[6 + d], (to, g))
    zall[rows(z * piece, piece), :] = zout[...]
    yield False
    for d in range(1, ZN):
        arrive(zall, 0, piece, zr.at[6 + d])
    for q in range(2):
        gath[rows(inner[q], second), :] = zall[q * second : (q + 1) * second, :]
        spread(1 - q, inner[q], second, 14 + 3 * q)
    yield True
    for q in range(2):
        for d in range(3):
            arrive(gath, 0, second, rsem.at[14 + 3 * q + d])
        spread(q, outer[q], first, 20 + 3 * q)
    yield False
    for q in range(2):
        for d in range(3):
            arrive(gath, 0, first, rsem.at[20 + 3 * q + d])
        here = pl.ds(q * colour, colour)
        go(gath.at[here], back.at[here], ssem.at[26 + q], rsem.at[26 + q], twin)
    yield False
    width = outs[0].shape[1]
    for k in range(half // width):
        if k % 2 == 0:
            arrive(back, (k // 2) * colour, colour, rsem.at[26 + k // 2])
        here = pl.ds(k * width, width)
        mine, theirs = gath[here, :], back[here, :]
        lanes = pl.ds(k * LANE, LANE)
        even = c == 0
        outs[0][layer, :, lanes] = jnp.where(even, mine, theirs)
        outs[1][layer, :, lanes] = jnp.where(even, theirs, mine)
    yield False


def step_kernel(
    col_in,
    idx_in,
    cnt_in,
    val_in,
    feat_in,
    cot_in,
    ws_in,
    wn_in,
    self_ref,
    neigh_ref,
    in_ref,
    col_ref,
    idx_ref,
    cnt_ref,
    val_ref,
    cot_ref,
    ws_ref,
    wn_ref,
    h,
    agg,
    pre,
    base,
    aggn,
    near,
    far,
    far_t,
    pick,
    pick_t,
    perm,
    out1,
    got1,
    out2,
    got2,
    full,
    part,
    other,
    got,
    gath,
    back,
    zin,
    zout,
    zgot,
    zall,
    s1,
    r1,
    s2,
    r2,
    ssem,
    rsem,
    zs,
    zr,
    load,
):
    z, g, x, y, c = place()
    node_rows, width = feat_in.shape
    layers = ws_in.shape[0]
    devices = idx_in.shape[1]
    halo = devices * idx_in.shape[0]
    tile = val_ref.shape[2]
    wide = width // 2
    zrow, grow = halo // ZN, halo // GN

    ys = [lax.rem(y + d, 4) for d in range(4)]
    cs = [c, 1 - c]

    loads = [
        pltpu.make_async_copy(src, dst, load.at[k])
        for k, (src, dst) in enumerate(
            (
                (idx_in, idx_ref),
                (cnt_in, cnt_ref),
                (feat_in, h.at[0]),
                (val_in, val_ref),
                (col_in, col_ref),
                (ws_in, ws_ref),
                (wn_in, wn_ref),
                (cot_in, cot_ref),
            )
        )
    ]
    for move in loads:
        move.start()
    bar = pltpu.get_barrier_semaphore()
    for d in range(1, ZN):
        pl.semaphore_signal(
            bar, inc=1, device_id=(lax.rem(z + d, ZN), g), device_id_type=MESH
        )

    def greet(px, own):
        for dy in range(4):
            for dc in range(2):
                if not (own and dy == 0 and dc == 0):
                    peer = (z, px * 8 + ys[dy] * 2 + cs[dc])
                    pl.semaphore_signal(bar, inc=1, device_id=peer, device_id_type=MESH)

    def greet_far(d, carry):
        greet(lax.rem(x + d, 4), False)
        return carry

    lax.fori_loop(1, 4, greet_far, 0)
    greet(x, True)

    i = lax.broadcasted_iota(jnp.int32, (halo, halo), 0)
    j = lax.broadcasted_iota(jnp.int32, (halo, halo), 1)

    def one_hot(target):
        return (j == target).astype(F32).astype(BF)

    node = lax.broadcasted_iota(jnp.int32, (node_rows, devices), 0)
    loads[0].wait()
    loads[1].wait()
    for s in range(halo // devices):
        row = jnp.where(s < cnt_ref[...], idx_ref[s : s + 1, :], -1)
        pick_t[0, :, s * devices : (s + 1) * devices] = (node == row).astype(F32).astype(BF)
    pick[0] = pick_t[0].T
    by_slot = pick[0]
    pick[1] = dot(one_hot((i & 1) * 256 + ((i >> 1) & 7) * 32 + (i >> 4)), by_slot).astype(BF)
    pick[0] = dot(one_hot((i & 1) * 256 + (i >> 1)), by_slot).astype(BF)
    loads[2].wait()

    def constants():
        perm[0] = one_hot(((i >> 1) & 7) * 64 + (i >> 4) * 2 + (i & 1))
        perm[1] = one_hot(((i >> 1) & 31) * 16 + (i >> 6) * 2 + (i & 1))
        for move in loads[3:]:
            move.wait()
        tiles_near = node_rows // tile
        for r in range(col_ref.shape[0]):
            for t in range(tiles_near + halo // tile):
                block = jnp.zeros((tile, tile), F32)
                for b in range(col_ref.shape[1]):
                    on = (col_ref[r, b] == t).astype(F32)
                    block = block + val_ref[r, b].astype(F32) * on
                at = slice(r * tile, (r + 1) * tile)
                if t < tiles_near:
                    near[at, t * tile : (t + 1) * tile] = block.astype(BF)
                else:
                    k = t - tiles_near
                    far[0, at, k * tile : (k + 1) * tile] = block.astype(BF)
        far[1] = dot(far[0], perm[1]).astype(BF)

    pl.semaphore_wait(bar, ZN - 1 + GN - 1)

    def send_z(src, dst, s, r):
        for d in (4, 3, 5, 2, 6, 1, 7):
            to = lax.rem(z + d, ZN)
            copy(
                src.at[rows(to * zrow, zrow)], dst.at[rows(z * zrow, zrow)], s, r, (to, g)
            ).start()
        dst[rows(z * zrow, zrow), :] = src[rows(z * zrow, zrow), :]

    def send_g(src, dst, s, r):
        def part(px, own):
            for dy in (2, 1, 3, 0):
                for dc in (1, 0):
                    if own and dy == 0 and dc == 0:
                        continue
                    to = px * 8 + ys[dy] * 2 + cs[dc]
                    copy(
                        src.at[rows(to * grow, grow)], dst.at[rows(g * grow, grow)], s, r, (z, to)
                    ).start()

        def body(d, carry):
            part(lax.rem(x + d, 4), False)
            return carry

        lax.fori_loop(1, 4, body, 0)
        part(x, True)
        dst[rows(g * grow, grow), :] = src[rows(g * grow, grow), :]

    def wait_z(dst, r):
        here = dst.at[pl.ds(0, halo - zrow)]
        copy(here, here, r, r, (z, g)).wait_recv()

    def wait_g(dst, r):
        here = dst.at[pl.ds(0, halo - grow)]
        copy(here, here, r, r, (z, g)).wait_recv()

    def start(t, left, right):
        out1[t, 0] = left()
        send_z(out1.at[t, 0], got1.at[t, 0], s1.at[t, 0], r1.at[t, 0])
        out1[t, 1] = right()
        send_g(out1.at[t, 1], got1.at[t, 1], s1.at[t, 1], r1.at[t, 1])

    def turn_right(t):
        wait_g(got1.at[t, 1], r1.at[t, 1])
        out2[t, 1] = dot(perm[1], got1[t, 1]).astype(BF)
        send_z(out2.at[t, 1], got2.at[t, 1], s2.at[t, 1], r2.at[t, 1])

    def turn_left(t):
        wait_z(got1.at[t, 0], r1.at[t, 0])
        out2[t, 0] = dot(perm[0], got1[t, 0]).astype(BF)
        send_g(out2.at[t, 0], got2.at[t, 0], s2.at[t, 0], r2.at[t, 0])

    def slope(v):
        sigma = jax.nn.sigmoid(v)
        return sigma * (1.0 + v * (1.0 - sigma))

    def forward(t, between):
        start(
            t,
            lambda: dot(pick[0], h[t, :, :wide]).astype(BF),
            lambda: dot(pick[1], h[t, :, wide:]).astype(BF),
        )
        between()
        base[...] = dot(h[t], ws_ref[t])
        aggn[...] = dot(near[...], h[t])
        turn_right(t)
        turn_left(t)
        wait_g(got2.at[t, 0], r2.at[t, 0])
        agg[t, :, :wide] = (aggn[:, :wide] + dot(far[1], got2[t, 0])).astype(BF)
        base[...] += dot(agg[t, :, :wide], wn_ref[t, :wide, :])
        wait_z(got2.at[t, 1], r2.at[t, 1])
        agg[t, :, wide:] = (aggn[:, wide:] + dot(far[0], got2[t, 1])).astype(BF)
        v = base[...] + dot(agg[t, :, wide:], wn_ref[t, wide:, :])
        pre[t] = v
        h[t + 1] = (v * jax.nn.sigmoid(v)).astype(BF)

    forward(0, constants)

    def later(t, carry):
        def between():
            pre[t - 1] = slope(pre[t - 1])

        forward(t, between)
        return carry

    lax.fori_loop(1, layers, later, 0)
    for k in range(2):
        far_t[k] = far[k].T
        pick_t[k] = pick[k].T

    outs = (self_ref, neigh_ref)
    bufs = (full, part, other, got, gath, back, zin, zout, zgot, zall)
    sems = (ssem, rsem, zs, zr)
    sends, running = [], []

    def advance(much=True, only=None):
        for entry in reversed(list(running)):
            run, layer, heavy = entry
            if (heavy and not much) or only not in (None, layer):
                continue
            entry[2] = next(run, None)
            if entry[2] is None:
                running.remove(entry)

    grad = cot_ref
    for at in range(layers - 1, -1, -1):
        t = 2 * layers - 1 - at
        if at == layers - 1:
            pre[at] = slope(pre[at])
        delta = (grad[...].astype(F32) * pre[at]).astype(BF)
        up = dot(delta, wn_ref[at], AGAINST).astype(BF)
        start(
            t,
            lambda: dot(far_t[0], up[:, :wide]).astype(BF),
            lambda: dot(far_t[1], up[:, wide:]).astype(BF),
        )
        for m, left in enumerate((h, agg)):
            for k in range(2):
                term = dot(left[at], delta[:, k * wide : (k + 1) * wide], TRANSPOSED).astype(BF)
                for n in range(wide // LANE):
                    full[at, pl.ds((m * 4 + k * 2 + n) * width, width), :] = term[
                        :, n * LANE : (n + 1) * LANE
                    ]
        running.append([sum_stages(at, outs, bufs, sems, sends), at, False])
        advance()
        base[...] = dot(delta, ws_ref[at], AGAINST) + dot(near[...], up, TRANSPOSED)
        if at == 0:
            advance()
        turn_right(t)
        turn_left(t)
        advance(much=False)
        advance(much=False)
        wait_g(got2.at[t, 0], r2.at[t, 0])
        in_ref[:, :wide] = (base[:, :wide] + dot(pick_t[1], got2[t, 0])).astype(BF)
        if at == 0:
            advance(only=0)
        wait_z(got2.at[t, 1], r2.at[t, 1])
        in_ref[:, wide:] = (base[:, wide:] + dot(pick_t[0], got2[t, 1])).astype(BF)
        grad = in_ref
    while running:
        advance()
    for move in sends:
        move.wait_send()

    def drain(t, carry):
        for k, (first, second) in enumerate(((zrow, grow), (grow, zrow))):
            for ref, sem, own in ((out1, s1, first), (out2, s2, second)):
                here = ref.at[t, k, pl.ds(0, halo - own)]
                copy(here, here, sem.at[t, k], sem.at[t, k], (z, g)).wait_send()
        return carry

    lax.fori_loop(0, 2 * layers, drain, 0)


def whole_step(col, idx, cnt, val, feat, cot, ws, wn):
    layers, width, _ = ws.shape
    node_rows, halo = feat.shape[0], idx.shape[0] * idx.shape[1]
    steps = 2 * layers
    total = 2 * width * width // LANE
    half = total // 2
    dma = pltpu.SemaphoreType.DMA
    vm = pltpu.VMEM

    grads = jax.ShapeDtypeStruct(ws.shape, BF)
    flow = vm((steps, 2, halo, width // 2), BF)
    return pl.pallas_call(
        step_kernel,
        out_shape=(grads, grads, jax.ShapeDtypeStruct(feat.shape, BF)),
        in_specs=[pl.BlockSpec(memory_space=pltpu.HBM)] * 8,
        out_specs=[pl.BlockSpec(memory_space=pltpu.VMEM)] * 3,
        scratch_shapes=[
            pltpu.SMEM(col.shape, col.dtype),
            vm(idx.shape, idx.dtype),
            vm(cnt.shape, cnt.dtype),
            vm(val.shape, BF),
            vm(cot.shape, BF),
            vm(ws.shape, BF),
            vm(wn.shape, BF),
            vm((layers + 1, node_rows, width), BF),
            vm((layers, node_rows, width), BF),
            vm((layers, node_rows, width), F32),
            vm((node_rows, width), F32),
            vm((node_rows, width), F32),
            vm((node_rows, node_rows), BF),
            vm((2, node_rows, halo), BF),
            vm((2, halo, node_rows), BF),
            vm((2, halo, node_rows), BF),
            vm((2, node_rows, halo), BF),
            vm((2, halo, halo), BF),
            flow,
            flow,
            flow,
            flow,
            vm((layers, total, LANE), BF),
            vm((layers, half, LANE), BF),
            vm((layers, half, LANE), BF),
            vm((layers, half * 15 // 16, LANE), BF),
            vm((layers, half, LANE), BF),
            vm((layers, half, LANE), BF),
            vm((layers, half // 16, LANE), BF),
            vm((layers, half // 128, LANE), BF),
            vm((layers, half // 128 * 7, LANE), BF),
            vm((layers, half // 16, LANE), BF),
            dma((steps, 2)),
            dma((steps, 2)),
            dma((steps, 2)),
            dma((steps, 2)),
            dma((layers, 28)),
            dma((layers, 28)),
            dma((layers, 14)),
            dma((layers, 14)),
            dma((8,)),
        ],
        compiler_params=pltpu.CompilerParams(
            collective_id=0, has_side_effects=True, vmem_limit_bytes=60 * 1024 * 1024
        ),
        name="whole_step",
    )(col, idx, cnt, val, feat, cot, ws, wn)


def per_device(
    features, cotangent, self_weight, neigh_weight, block_val, block_col, send_idx, send_count
):
    devices = lax.axis_size("gx") * lax.axis_size("gy")
    slots = send_idx.shape[2]
    scale = 1.0 / math.sqrt(features.shape[0] * devices)
    self_sum, neigh_sum, grad = whole_step(
        block_col,
        send_idx.reshape(devices, slots).T,
        send_count,
        block_val,
        features,
        cotangent,
        self_weight,
        neigh_weight,
    )

    def scaled(total):
        return (total.astype(F32) * scale).astype(BF)

    return scaled(self_sum), scaled(neigh_sum), grad


def solution(mesh):
    return jax.shard_map(
        per_device,
        mesh=mesh,
        in_specs=(
            P(("gx", "gy"), None),
            P(("gx", "gy"), None),
            P(),
            P(),
            P(("gx", "gy"), None, None, None),
            P(("gx", "gy"), None),
            P(("gx", "gy"), None, None),
            P(("gx", "gy"), None),
        ),
        out_specs=(P(), P(), P(("gx", "gy"), None)),
        check_vma=False,
    )
```
